32 devices in a mesh: img: 2 (over x), rows: 16 (over z, y, core).
Axes of the slice: x: 2, y: 2, z: 4, core: 2. Of those that a mesh axis runs over, the one named last changes fastest.
Arguments:
- image: bfloat16 [128, 256, 512], P(('img', 'rows')), parts along dimension 0, may hold values from -32 to 32
- gain_in: float32 [512], replicated, may hold values from 0.1 to 1.9
- shift_in: float32 [512], replicated, may hold values from -3 to 3
- conv_in: bfloat16 [3, 3, 512, 512], replicated, may hold values from -0.09375 to 0.09375
- gain_mid: float32 [512], replicated, may hold values from 0.1 to 1.9
- shift_mid: float32 [512], replicated, may hold values from -3 to 3
- conv_out: bfloat16 [3, 3, 512, 512], replicated, may hold values from -0.09375 to 0.09375
- bias_out: float32 [512], replicated, may hold values from -2 to 2
Outputs:
- result: bfloat16 [128, 256, 512], P(('img', 'rows')), parts along dimension 0
The draws below stay inside these ranges and needn't reach their ends.
There are 2 independent parts, one for each index of `img`. The reference program is written for one: setup_inputs(seed, part) draws one part's arguments, and reference() takes and returns one part's arrays. A program takes and returns all parts, laid end to end along the dimension named above; an argument that names none is the same for every part. Nothing has to cross between parts.
All inputs are finite; a program needn't handle non-finite values.
Results may differ from the reference program's by a relative error of at most 0.0045.
Values may be sent and summed in bfloat16 or wider, within the bound.
A program may use at most 64 MiB of HBM per device.

```python
import math
import jax
import jax.numpy as jnp
from jax import lax

C = 512
GROUPS = 32
COLS = 256
PICTURE_HEIGHT = 64


def draw_image(key, part):
    sampler_seeds = jax.random.split(key, 8)
    row_pos = jnp.arange(PICTURE_HEIGHT, dtype=jnp.float32) / max(PICTURE_HEIGHT - 1, 1)
    flip = jax.random.uniform(sampler_seeds[4], (), jnp.float32)
    toward = jnp.where(flip < 0.5, row_pos, 1.0 - row_pos)
    log_ratio = jax.random.uniform(sampler_seeds[5], (), jnp.float32, math.log(3.0), math.log(9.0))
    smooth_drift_surface = 1.4 * jnp.exp((toward - 1.0) * log_ratio)
    jagged_surface = jnp.exp(jax.random.uniform(sampler_seeds[6], (PICTURE_HEIGHT,), jnp.float32, math.log(0.7), math.log(1.4)))
    sudden_spike_perturbation = jnp.where(jax.random.uniform(sampler_seeds[7], (PICTURE_HEIGHT,), jnp.float32) < 0.0625, 1.6, 1.0)
    vertical_multiplier = smooth_drift_surface * jagged_surface * sudden_spike_perturbation
    col_scale = jnp.exp(jax.random.uniform(sampler_seeds[0], (COLS,), jnp.float32, math.log(0.3), math.log(3.0)))
    channel_scale_factor = jnp.exp(jax.random.uniform(sampler_seeds[1], (C,), jnp.float32, math.log(0.7), math.log(1.4)))
    noise = jnp.clip(jax.random.normal(sampler_seeds[2], (PICTURE_HEIGHT, COLS, C), jnp.float32), -4.0, 4.0)
    offset = 0.3 * jax.random.normal(sampler_seeds[3], (C,), jnp.float32)
    value_entries = offset + vertical_multiplier[:, None, None] * col_scale[None, :, None] * channel_scale_factor * noise
    return jnp.clip(value_entries, -32.0, 32.0).astype(jnp.bfloat16)


def normal_values(key, dims, deviation, reach, held_as=jnp.bfloat16):
    array = deviation * jax.random.normal(key, dims, jnp.float32)
    return jnp.clip(array, min=-reach, max=reach).astype(held_as)


def setup_inputs(seed: int = 0, part: int = 0) -> dict:
    arg_keys = jax.random.split(jax.random.key(seed), 9)
    own_keys = jax.random.split(jax.random.fold_in(arg_keys[8], part), 9)
    return {
        "image": draw_image(jax.random.fold_in(jax.random.fold_in(arg_keys[8], part), 71), part),
        "gain_in": jnp.clip(1.0 + 0.18 * jax.random.normal(arg_keys[1], (C,), jnp.float32), 0.1, 1.9),
        "shift_in": normal_values(arg_keys[2], (C,), 0.5, 3.0, jnp.float32),
        "conv_in": normal_values(arg_keys[3], (3, 3, C, C), (9 * C) ** -0.5, 0.09375),
        "gain_mid": jnp.clip(1.0 + 0.18 * jax.random.normal(arg_keys[4], (C,), jnp.float32), 0.1, 1.9),
        "shift_mid": normal_values(arg_keys[5], (C,), 0.5, 3.0, jnp.float32),
        "conv_out": normal_values(arg_keys[6], (3, 3, C, C), (9 * C) ** -0.5, 0.09375),
        "bias_out": normal_values(arg_keys[7], (C,), 0.3, 2.0, jnp.float32),
    }


def normalize_silu(value_entries, gain, shift):
    height, width, chans = value_entries.shape
    grouped = value_entries.reshape(height, width, GROUPS, chans // GROUPS)
    midpoint_location = lax.optimization_barrier(jnp.mean(grouped, axis=(0, 1, 3), keepdims=True))
    spread = lax.optimization_barrier(jnp.mean((grouped - midpoint_location) ** 2, axis=(0, 1, 3), keepdims=True))
    scaled = ((grouped - midpoint_location) / jnp.sqrt(spread + 1e-06)).reshape(height, width, chans)
    return jax.nn.silu(scaled * gain + shift).astype(jnp.bfloat16)

def convolve(active, kernel):
    output = lax.conv_general_dilated(active[None].astype(jnp.float32), kernel.astype(jnp.float32), (1, 1), 'SAME', dimension_numbers=('NHWC', 'HWIO', 'NHWC'), precision=lax.Precision.HIGHEST)
    return output[0]

def reference(image, gain_in, shift_in, conv_in, gain_mid, shift_mid, conv_out, bias_out):
    first = normalize_silu(image.astype(jnp.float32), gain_in, shift_in)
    middle = convolve(first, conv_in).astype(jnp.bfloat16)
    latter_operand = normalize_silu(middle.astype(jnp.float32), gain_mid, shift_mid)
    total = image.astype(jnp.float32) + convolve(latter_operand, conv_out) + bias_out
    return total.astype(jnp.bfloat16)
```

```python
import functools

import jax
import jax.numpy as jnp
from jax import lax
from jax.experimental import pallas as pl
from jax.experimental.pallas import tpu as pltpu
from jax.sharding import PartitionSpec as P

GROUPS = 32
LANES = 128
SIDE = 256
UNITS = 2
CHUNK = 32
MESH = pl.DeviceIdType.MESH
BF16, F32 = jnp.bfloat16, jnp.float32


def packed(sums, squares):
    chans = sums.shape[1]
    pieces = [part[:, k : k + LANES] for part in (sums, squares) for k in range(0, chans, LANES)]
    return jnp.concatenate(pieces, axis=0)


def flat(tile):
    return jnp.concatenate([tile[k : k + 1] for k in range(tile.shape[0])], axis=1)


def group_total(tile, size):
    lane = lax.broadcasted_iota(jnp.int32, tile.shape, 1)
    step = 1
    while step < size:
        up = pltpu.roll(tile, step, 1)
        down = pltpu.roll(tile, LANES - step, 1)
        tile = tile + jnp.where((lane & step) != 0, up, down)
        step *= 2
    return tile


def kernel(n, image, gain_in, shift_in, conv_in, gain_mid, shift_mid, conv_out, bias_out, out,
           img, act, mid, w_in, w_out, vec, sums, gath_in, gath_mid,
           img_sem, load_sem, halo_send, halo_recv, stat_send, stat_recv):
    me = lax.axis_index("rows")
    height, width, chans = image.shape
    size = chans // GROUPS
    count = float(height * width * size * n)
    parts = chans // LANES
    depth = chans // SIDE

    order = [0, height - 1] + list(range(1, height - 1))
    loads = {
        r: pltpu.make_async_copy(image.at[r], img.at[1 + r], img_sem.at[r]) for r in order
    }
    for r in order:
        loads[r].start()
    load_w_in = pltpu.make_async_copy(conv_in, w_in, load_sem.at[0])
    load_w_in.start()
    for k, source in enumerate((gain_in, shift_in, gain_mid, shift_mid, bias_out)):
        pltpu.make_async_copy(source, vec.at[pl.ds(k, 1)], load_sem.at[2]).start()
    load_w_out = pltpu.make_async_copy(conv_out, w_out, load_sem.at[1])
    load_w_out.start()

    barrier = pltpu.get_barrier_semaphore()
    for d in range(1, n):
        pl.semaphore_signal(
            barrier, inc=1, device_id={"rows": lax.rem(me + d, n)}, device_id_type=MESH
        )

    def add_stats(value, lanes):
        folded = value.reshape(value.shape[0] // 8, 8, value.shape[1])
        sums[0, :, lanes] += jnp.sum(folded, axis=0)
        sums[1, :, lanes] += jnp.sum(folded * folded, axis=0)

    def stat_copy(gath, which, d):
        return pltpu.make_async_remote_copy(
            src_ref=gath.at[pl.ds(0, 1)],
            dst_ref=gath.at[pl.ds(d, 1)],
            send_sem=stat_send.at[which],
            recv_sem=stat_recv.at[which],
            device_id={"rows": lax.rem(me + d, n)},
            device_id_type=MESH,
        )

    def send_stats(gath, which):
        tile = packed(
            jnp.sum(sums[0], axis=0, keepdims=True), jnp.sum(sums[1], axis=0, keepdims=True)
        )
        tile = group_total(tile, size)
        lane = lax.broadcasted_iota(jnp.int32, tile.shape, 1)
        row = lax.broadcasted_iota(jnp.int32, tile.shape, 0)
        mine = jnp.where(lax.rem(lane, size) == row, tile, 0.0)
        gath[0:1] = jnp.sum(mine, axis=0, keepdims=True)
        for d in range(1, n):
            stat_copy(gath, which, d).start()

    def all_sent(gath, which):
        pltpu.make_async_copy(
            gath.at[pl.ds(1, n - 1)], gath.at[pl.ds(1, n - 1)], stat_send.at[which]
        ).wait()

    def receive_stats(gath, which, gain, shift):
        pltpu.make_async_copy(
            gath.at[pl.ds(1, n - 1)], gath.at[pl.ds(1, n - 1)], stat_recv.at[which]
        ).wait()
        total = jnp.sum(gath[...], axis=0, keepdims=True) / count
        total = jnp.broadcast_to(total, (2 * parts, LANES))
        lane = lax.broadcasted_iota(jnp.int32, total.shape, 1)
        row = lax.broadcasted_iota(jnp.int32, total.shape, 0)
        tile = jnp.take_along_axis(total, lane - lax.rem(lane, size) + row, axis=1)
        mean, square = tile[:parts], tile[parts:]
        variance = jnp.maximum(square - mean * mean, 0.0)
        scale = flat(lax.rsqrt(variance + 1e-06)) * (0.5 * gain)
        return scale, 0.5 * shift - flat(mean) * scale

    def halo_copies(buf, which):
        up = pltpu.make_async_remote_copy(
            src_ref=buf.at[1],
            dst_ref=buf.at[height + 1],
            send_sem=halo_send.at[which, 0],
            recv_sem=halo_recv.at[which, 0],
            device_id={"rows": jnp.maximum(me - 1, 0)},
            device_id_type=MESH,
        )
        down = pltpu.make_async_remote_copy(
            src_ref=buf.at[height],
            dst_ref=buf.at[0],
            send_sem=halo_send.at[which, 1],
            recv_sem=halo_recv.at[which, 1],
            device_id={"rows": jnp.minimum(me + 1, n - 1)},
            device_id_type=MESH,
        )
        return up, down

    def send_halo(buf, which):
        up, down = halo_copies(buf, which)

        @pl.when(me > 0)
        def _():
            up.start()

        @pl.when(me < n - 1)
        def _():
            down.start()

    def wait_halo(buf, which):
        up, down = halo_copies(buf, which)

        @pl.when(me > 0)
        def _():
            up.wait_send()
            down.wait_recv()

        @pl.when(me < n - 1)
        def _():
            down.wait_send()
            up.wait_recv()

    def activate(buf, row, k, scale, shift, inside=None):
        lanes = slice(k * LANES, (k + 1) * LANES)
        half = buf[row, :, lanes].astype(F32) * scale[:, lanes] + shift[:, lanes]
        value = half + half * jnp.tanh(half)
        if inside is not None:
            value = jnp.where(inside, value, 0.0)
        col = lax.broadcasted_iota(jnp.int32, value.shape, 0)
        act[1, row, :, lanes] = value.astype(BF16)
        left = jnp.where(col == 0, 0.0, pltpu.roll(value, 1, 0))
        act[0, row, :, lanes] = left.astype(BF16)
        right = jnp.where(col == width - 1, 0.0, pltpu.roll(value, width - 1, 0))
        act[2, row, :, lanes] = right.astype(BF16)

    def body(*accs):
        acc = [accs[q * height : (q + 1) * height] for q in range(UNITS)]

        zero = jnp.zeros((SIDE, SIDE), BF16)
        for q in range(UNITS):
            for s in range(2):
                pltpu.matmul_acc_lhs(acc[q][0], zero, load_staged_rhs=s)
        for q in range(UNITS):
            for r in range(height):
                pltpu.matmul_pop(acc[q][r])

        def contract(weights, steps, hook=lambda t: None):
            def push(t):
                i, j, k = steps[t][:3]
                for q in range(UNITS):
                    pltpu.matmul_push_rhs(
                        weights[i, j, k * SIDE : (k + 1) * SIDE, q * SIDE : (q + 1) * SIDE],
                        staging_register=t % 2,
                        mxu_index=q,
                    )

            push(0)
            for t, (i, j, k, rows) in enumerate(steps):
                if t + 1 < len(steps):
                    push(t + 1)
                hook(t)
                for m, r in enumerate(rows):
                    left = act[j, r + i, :, k * SIDE : (k + 1) * SIDE]
                    for q in range(UNITS):
                        pltpu.matmul_acc_lhs(
                            acc[q][r], left, load_staged_rhs=t % 2 if m == 0 else None
                        )

        own = [
            (i, j, k, [r for r in range(height) if 1 <= r + i <= height])
            for k in range(depth)
            for i in (1, 0, 2)
            for j in range(3)
        ]
        ends = [
            (i, j, k, [r]) for i, r in ((0, 0), (2, height - 1))
            for k in range(depth) for j in range(3)
        ]
        slabs = SIDE // LANES

        def convolve(buf, which, weights, scale, shift, finish):
            pieces = [
                (r, k) for k in range(parts) for r in range(1, height + 1)
            ]
            early = height * slabs
            for r, k in pieces[:early]:
                activate(buf, r, k, scale, shift)
            rest = pieces[early:]

            def hook(t):
                if rest:
                    r, k = rest.pop(0)
                    activate(buf, r, k, scale, shift)

            contract(weights, own, hook)
            assert not rest
            for r in range(1, height - 1):
                finish(acc, r)
            wait_halo(buf, which)
            for k in range(parts):
                activate(buf, 0, k, scale, shift, me > 0)
                activate(buf, height + 1, k, scale, shift, me < n - 1)
            contract(weights, ends)
            for r in (0, height - 1):
                finish(acc, r)

        sums[...] = jnp.zeros_like(sums)
        for r in order:
            loads[r].wait()

        def stats_step(k, _):
            cols = pl.ds(pl.multiple_of(k * CHUNK, CHUNK), CHUNK)
            for r in range(height):
                add_stats(img[1 + r, cols].astype(F32), slice(None))
            return 0

        lax.fori_loop(0, width // CHUNK, stats_step, 0)
        pl.semaphore_wait(barrier, n - 1)
        send_stats(gath_in, 0)
        send_halo(img, 0)
        sums[...] = jnp.zeros_like(sums)
        load_w_in.wait()
        pltpu.make_async_copy(vec.at[pl.ds(0, 5)], vec.at[pl.ds(0, 5)], load_sem.at[2]).wait()
        scale, shift = receive_stats(gath_in, 0, vec[0:1], vec[1:2])

        def keep(acc, r):
            for q in range(UNITS):
                lanes = slice(q * SIDE, (q + 1) * SIDE)
                value = pltpu.matmul_pop(acc[q][r]).astype(BF16)
                mid[1 + r, :, lanes] = value
                add_stats(value.astype(F32), lanes)

        convolve(img, 0, w_in, scale, shift, keep)
        send_stats(gath_mid, 1)
        send_halo(mid, 1)
        load_w_out.wait()
        scale, shift = receive_stats(gath_mid, 1, vec[2:3], vec[3:4])

        def give(acc, r):
            for q in range(UNITS):
                lanes = slice(q * SIDE, (q + 1) * SIDE)
                value = pltpu.matmul_pop(acc[q][r]) + vec[4:5, lanes]
                out[r, :, lanes] = (img[1 + r, :, lanes].astype(F32) + value).astype(BF16)

        convolve(mid, 1, w_out, scale, shift, give)
        all_sent(gath_in, 0)
        all_sent(gath_mid, 1)

    pl.run_scoped(
        body, *[pltpu.ACC(q)((width, SIDE), F32) for q in range(UNITS) for _ in range(height)]
    )


def pin(x):
    return pltpu.with_memory_space_constraint(x, pltpu.HBM)


def local(n, image, gain_in, shift_in, conv_in, gain_mid, shift_mid, conv_out, bias_out):
    height, width, chans = image.shape
    whole = pl.BlockSpec(memory_space=pltpu.HBM)
    operands = (image, gain_in[None], shift_in[None], conv_in, gain_mid[None], shift_mid[None],
                conv_out, bias_out[None])
    return pl.pallas_call(
        functools.partial(kernel, n),
        out_shape=jax.ShapeDtypeStruct(image.shape, image.dtype),
        in_specs=[whole] * len(operands),
        out_specs=pl.BlockSpec(memory_space=pltpu.VMEM),
        scratch_shapes=[
            pltpu.VMEM((height + 2, width, chans), BF16),
            pltpu.VMEM((3, height + 2, width, chans), BF16),
            pltpu.VMEM((height + 2, width, chans), BF16),
            pltpu.VMEM(conv_in.shape, BF16),
            pltpu.VMEM(conv_out.shape, BF16),
            pltpu.VMEM((8, chans), F32),
            pltpu.VMEM((2, 8, chans), F32),
            pltpu.VMEM((n, LANES), F32),
            pltpu.VMEM((n, LANES), F32),
            pltpu.SemaphoreType.DMA((height,)),
            pltpu.SemaphoreType.DMA((3,)),
            pltpu.SemaphoreType.DMA((2, 2)),
            pltpu.SemaphoreType.DMA((2, 2)),
            pltpu.SemaphoreType.DMA((2,)),
            pltpu.SemaphoreType.DMA((2,)),
        ],
        compiler_params=pltpu.CompilerParams(
            collective_id=0, has_side_effects=True, vmem_limit_bytes=40 * 1024 * 1024
        ),
    )(*[pin(x) for x in operands])


def solution(mesh):
    n = mesh.shape["rows"]
    in_specs = (P(("img", "rows"), None, None), P(), P(), P(), P(), P(), P(), P())
    out_specs = P(("img", "rows"), None, None)
    return jax.shard_map(
        functools.partial(local, n), mesh=mesh, in_specs=in_specs, out_specs=out_specs,
        check_vma=False,
    )
```

```python
import functools

import jax
import jax.numpy as jnp
from jax import lax
from jax.experimental import pallas as pl
from jax.experimental.pallas import tpu as pltpu
from jax.sharding import PartitionSpec as P

GROUPS = 32
LANES = 128
SIDE = 256
UNITS = 2
CHUNK = 32
LEAD = 3
TAIL = 3
MESH = pl.DeviceIdType.MESH
BF16, F32 = jnp.bfloat16, jnp.float32


def packed(sums, squares):
    chans = sums.shape[1]
    pieces = [part[:, k : k + LANES] for part in (sums, squares) for k in range(0, chans, LANES)]
    return jnp.concatenate(pieces, axis=0)


def flat(tile):
    return jnp.concatenate([tile[k : k + 1] for k in range(tile.shape[0])], axis=1)


def group_total(tile, size):
    lane = lax.broadcasted_iota(jnp.int32, tile.shape, 1)
    step = 1
    while step < size:
        up = pltpu.roll(tile, step, 1)
        down = pltpu.roll(tile, LANES - step, 1)
        tile = tile + jnp.where((lane & step) != 0, up, down)
        step *= 2
    return tile


def kernel(n, image, gain_in, shift_in, conv_in, gain_mid, shift_mid, conv_out, bias_out, out,
           img, act, mid, w_in, w_out, taps, mixed, part, vec, sums, gath_in, gath_a, gath_b,
           img_sem, load_sem, halo_send, halo_recv, stat_send, stat_recv):
    me = lax.axis_index("rows")
    height, width, chans = image.shape
    size = chans // GROUPS
    count = float(height * width * size * n)
    parts = chans // LANES
    depth = chans // SIDE
    slabs = SIDE // LANES
    share = height // UNITS

    order = [0, height - 1] + list(range(1, height - 1))
    loads = {
        r: pltpu.make_async_copy(image.at[r], img.at[1 + r], img_sem.at[r]) for r in order
    }
    for r in order:
        loads[r].start()
    load_w_in = pltpu.make_async_copy(conv_in, w_in, load_sem.at[0])
    load_w_out = pltpu.make_async_copy(conv_out, w_out, load_sem.at[1])

    barrier = pltpu.get_barrier_semaphore()
    for d in range(1, n):
        pl.semaphore_signal(
            barrier, inc=1, device_id={"rows": lax.rem(me + d, n)}, device_id_type=MESH
        )

    def add_stats(value, lanes):
        folded = value.reshape(value.shape[0] // 8, 8, value.shape[1])
        sums[0, :, lanes] += jnp.sum(folded, axis=0)
        sums[1, :, lanes] += jnp.sum(folded * folded, axis=0)

    def stat_copy(gath, which, d):
        return pltpu.make_async_remote_copy(
            src_ref=gath.at[pl.ds(0, 1)],
            dst_ref=gath.at[pl.ds(d, 1)],
            send_sem=stat_send.at[which],
            recv_sem=stat_recv.at[which],
            device_id={"rows": lax.rem(me + d, n)},
            device_id_type=MESH,
        )

    def prepare_stats(gath, lanes):
        tile = packed(
            jnp.sum(sums[0, :, lanes], axis=0, keepdims=True),
            jnp.sum(sums[1, :, lanes], axis=0, keepdims=True),
        )
        tile = group_total(tile, size)
        lane = lax.broadcasted_iota(jnp.int32, tile.shape, 1)
        row = lax.broadcasted_iota(jnp.int32, tile.shape, 0)
        mine = jnp.where(lax.rem(lane, size) == row, tile, 0.0)
        gath[0:1] = jnp.sum(mine, axis=0, keepdims=True)

    def send_stats(gath, which):
        for d in range(1, n):
            stat_copy(gath, which, d).start()

    def all_sent(gath, which):
        pltpu.make_async_copy(
            gath.at[pl.ds(1, n - 1)], gath.at[pl.ds(1, n - 1)], stat_send.at[which]
        ).wait()

    def receive_stats(gath, which, gain, shift):
        pltpu.make_async_copy(
            gath.at[pl.ds(1, n - 1)], gath.at[pl.ds(1, n - 1)], stat_recv.at[which]
        ).wait()
        pieces = gain.shape[1] // LANES
        total = jnp.sum(gath[...], axis=0, keepdims=True) / count
        total = jnp.broadcast_to(total, (2 * pieces, LANES))
        lane = lax.broadcasted_iota(jnp.int32, total.shape, 1)
        row = lax.broadcasted_iota(jnp.int32, total.shape, 0)
        tile = jnp.take_along_axis(total, lane - lax.rem(lane, size) + row, axis=1)
        mean, square = tile[:pieces], tile[pieces:]
        variance = jnp.maximum(square - mean * mean, 0.0)
        scale = flat(lax.rsqrt(variance + 1e-06)) * (0.5 * gain)
        return scale, 0.5 * shift - flat(mean) * scale

    def halo_copies(buf, which, lanes):
        up = pltpu.make_async_remote_copy(
            src_ref=buf.at[1, :, lanes],
            dst_ref=buf.at[height + 1, :, lanes],
            send_sem=halo_send.at[which, 0],
            recv_sem=halo_recv.at[which, 0],
            device_id={"rows": jnp.maximum(me - 1, 0)},
            device_id_type=MESH,
        )
        down = pltpu.make_async_remote_copy(
            src_ref=buf.at[height, :, lanes],
            dst_ref=buf.at[0, :, lanes],
            send_sem=halo_send.at[which, 1],
            recv_sem=halo_recv.at[which, 1],
            device_id={"rows": jnp.minimum(me + 1, n - 1)},
            device_id_type=MESH,
        )
        return up, down

    def send_halo(buf, which, lanes):
        up, down = halo_copies(buf, which, lanes)

        @pl.when(me > 0)
        def _():
            up.start()

        @pl.when(me < n - 1)
        def _():
            down.start()

    def wait_halo(buf, which, lanes):
        up, down = halo_copies(buf, which, lanes)

        @pl.when(me > 0)
        def _():
            up.wait_send()
            down.wait_recv()

        @pl.when(me < n - 1)
        def _():
            down.wait_send()
            up.wait_recv()

    def activated(buf, row, k, affine):
        lanes = slice(k * LANES, (k + 1) * LANES)
        scale, shift = affine[k]
        half = buf[row, :, lanes].astype(F32) * scale + shift
        value = half + half * jnp.tanh(half)
        if row == 0:
            value = jnp.where(me > 0, value, 0.0)
        if row == height + 1:
            value = jnp.where(me < n - 1, value, 0.0)
        return value

    def store_shifted(target, value, row, lanes):
        col = lax.broadcasted_iota(jnp.int32, value.shape, 0)
        target[1, row, :, lanes] = value.astype(BF16)
        left = jnp.where(col == 0, 0.0, pltpu.roll(value, 1, 0))
        target[0, row, :, lanes] = left.astype(BF16)
        right = jnp.where(col == width - 1, 0.0, pltpu.roll(value, width - 1, 0))
        target[2, row, :, lanes] = right.astype(BF16)

    def activate(buf, row, k, affine):
        value = activated(buf, row, k, affine)
        store_shifted(act, value, row, slice(k * LANES, (k + 1) * LANES))

    def activate_plain(buf, row, k, affine):
        act[1, row, :, k * LANES : (k + 1) * LANES] = activated(buf, row, k, affine).astype(BF16)

    def mix_rows(m, a, b, sign, k, base):
        lanes = slice(k * LANES, (k + 1) * LANES)
        value = act[1, a, :, lanes].astype(F32) + sign * act[1, b, :, lanes].astype(F32)
        store_shifted(mixed, value, m, slice((k - base) * LANES, (k - base + 1) * LANES))

    def mix_taps(base):
        def step(t, _):
            rows = pl.ds(pl.multiple_of(t * CHUNK, CHUNK), CHUNK)
            source = pl.ds(pl.multiple_of(base + t * CHUNK, CHUNK), CHUNK)
            for j in range(3):
                ends = 0.5 * (
                    w_out[0, j, source].astype(F32) + w_out[2, j, source].astype(F32)
                )
                centre = 0.5 * w_out[1, j, source].astype(F32)
                taps[0, j, rows] = (ends + centre).astype(BF16)
                taps[1, j, rows] = (ends - centre).astype(BF16)
            return 0

        lax.fori_loop(0, SIDE // CHUNK, step, 0)

    def body(*accs):
        acc = [accs[q * height : (q + 1) * height] for q in range(UNITS)]

        zero = jnp.zeros((SIDE, SIDE), BF16)
        for q in range(UNITS):
            for s in range(2):
                pltpu.matmul_acc_lhs(acc[q][0], zero, load_staged_rhs=s)
        for q in range(UNITS):
            for r in range(height):
                pltpu.matmul_pop(acc[q][r])

        def contract(steps, hooks=None):
            def push(t):
                for q, (tile, _) in steps[t].items():
                    pltpu.matmul_push_rhs(tile(), staging_register=t % 2, mxu_index=q)

            push(0)
            for t, step in enumerate(steps):
                if t + 1 < len(steps):
                    push(t + 1)
                for hook in (hooks or {}).get(t, []):
                    hook()
                for m in range(height):
                    for q, (_, pairs) in step.items():
                        if m < len(pairs):
                            ref, left = pairs[m]
                            pltpu.matmul_acc_lhs(
                                acc[q][ref], left(), load_staged_rhs=t % 2 if m == 0 else None
                            )

        def tile_of(weights, i, j, k, p):
            return lambda: weights[
                i, j, k * SIDE : (k + 1) * SIDE, p * SIDE : (p + 1) * SIDE
            ]

        def left_of(j, row, k):
            return lambda: act[j, row, :, k * SIDE : (k + 1) * SIDE]

        spots = [(i, j) for j in range(3) for i in (1, 0, 2)]

        def inner(i, rows):
            return [r for r in rows if 1 <= r + i <= height]

        def place(p, r):
            return r // share, p * share + r % share

        def rows_split(w, p, k):
            def entry(i, j, q):
                rows = inner(i, range(q * share, (q + 1) * share))
                pairs = [(place(p, r)[1], left_of(j, r + i, k)) for r in rows]
                return tile_of(w, i, j, k, p), pairs

            own = [{q: entry(i, j, q) for q in range(UNITS)} for i, j in spots]
            ends = [
                {
                    q: (tile_of(w, i, j, k, p), [(place(p, r)[1], left_of(j, r + i, k))])
                    for q, i, r in ((0, 0, 0), (UNITS - 1, 2, height - 1))
                }
                for j in range(3)
            ]
            return own, ends

        def rows_first(w, p, k):
            queues = []
            for q in range(UNITS):
                rows = list(range(q * share, (q + 1) * share))
                inputs = range(1, height + 1) if q == 0 else range(height, 0, -1)
                queues.append([
                    (tile_of(w, x - r, j, k, p), [(place(p, r)[1], left_of(j, x, k))])
                    for x in inputs
                    for j in range(3)
                    for r in (rows if q == 0 else rows[::-1])
                    if 0 <= x - r <= 2
                ])
            return [dict(enumerate(step)) for step in zip(*queues, strict=True)]

        def chans_split(w, k):
            own = [
                {
                    q: (tile_of(w, i, j, k, q),
                        [(r, left_of(j, r + i, k)) for r in inner(i, range(height))])
                    for q in range(UNITS)
                }
                for i, j in spots
            ]
            ends = [
                {q: (tile_of(w, i, j, k, q), [(r, left_of(j, r + i, k))]) for q in range(UNITS)}
                for i, r in ((0, 0), (2, height - 1))
                for j in range(3)
            ]
            return own, ends

        def spread(hooks, first, last):
            assert first < last
            steps = range(first, last)
            plan = {t: [] for t in steps}
            for m, hook in enumerate(hooks):
                plan[first + m * len(steps) // len(hooks)].append(hook)
            return plan

        def lanes_of(p):
            return slice(p * SIDE, (p + 1) * SIDE)

        def rows_act(buf, rows, ks, affine):
            return [
                functools.partial(activate, buf, r, k, affine) for k in ks for r in rows
            ]

        def affine_of(pair, first=0):
            scale, shift = pair
            return {
                first + k: (scale[:, k * LANES : (k + 1) * LANES], shift[:, k * LANES : (k + 1) * LANES])
                for k in range(scale.shape[1] // LANES)
            }

        mine = range(1, height + 1)
        halo = (0, height + 1)

        sums[...] = jnp.zeros_like(sums)
        def stats_step(r, k, _):
            cols = pl.ds(pl.multiple_of(k * CHUNK, CHUNK), CHUNK)
            add_stats(img[1 + r, cols].astype(F32), slice(None))
            return 0

        for r in order:
            loads[r].wait()
            if r == order[-1]:
                for k, source in enumerate((gain_in, shift_in, gain_mid, shift_mid, bias_out)):
                    pltpu.make_async_copy(source, vec.at[pl.ds(k, 1)], load_sem.at[2]).start()
                load_w_in.start()
                load_w_out.start()
            lax.fori_loop(0, width // CHUNK, functools.partial(stats_step, r), 0)
        prepare_stats(gath_in, slice(None))
        pl.semaphore_wait(barrier, n - 1)
        send_stats(gath_in, 0)
        send_halo(img, 0, slice(None))
        sums[...] = jnp.zeros_like(sums)
        load_w_in.wait()
        load_w_out.wait()
        mix_taps(SIDE)
        pltpu.make_async_copy(vec.at[pl.ds(0, 5)], vec.at[pl.ds(0, 5)], load_sem.at[2]).wait()
        affine = affine_of(receive_stats(gath_in, 0, vec[0:1], vec[1:2]))

        def keep(p, r):
            lanes = lanes_of(p)
            q, ref = place(p, r)
            value = pltpu.matmul_pop(acc[q][ref]).astype(BF16)
            mid[1 + r, :, lanes] = value
            add_stats(value.astype(F32), lanes)

        middle = range(1, height - 1)
        outer = (0, height - 1)

        def kept(p, rows):
            return [functools.partial(keep, p, r) for r in rows]

        def both(p):
            first = [rows_split(w_in, p, k) for k in range(depth)]
            return [sum((pair[m] for pair in first), []) for m in range(2)]

        own_b, ends_b = both(1)
        _, ends_a = both(0)
        near = (1, height)
        far = [r for r in mine if r not in near]
        for hook in rows_act(img, near, range(slabs), affine):
            hook()
        start = rows_first(w_in, 0, 0)
        plan = spread(rows_act(img, far, range(slabs), affine), 0, 4)
        plan.update(spread(rows_act(img, mine, range(slabs, parts), affine), 4, len(start)))
        contract(start, plan)
        later = sum((rows_split(w_in, 0, k)[0] for k in range(1, depth)), [])
        contract(later[:-TAIL])
        wait_halo(img, 0, slice(None))
        contract(later[-TAIL:], spread(rows_act(img, halo, range(parts), affine), 0, TAIL))
        contract(ends_a, spread(kept(0, middle), 2, len(ends_a)))
        contract(
            own_b[:LEAD],
            spread(kept(0, outer) + [functools.partial(prepare_stats, gath_a, lanes_of(0))], 0, LEAD),
        )
        send_stats(gath_a, 1)
        send_halo(mid, 1, lanes_of(0))
        contract(own_b[LEAD:])
        contract(ends_b, spread(kept(1, middle), 1, len(ends_b)))
        for hook in kept(1, outer):
            hook()
        prepare_stats(gath_b, lanes_of(1))
        send_stats(gath_b, 2)
        send_halo(mid, 2, lanes_of(1))

        def give(r, ref):
            for q in range(UNITS):
                lanes = lanes_of(q)
                value = pltpu.matmul_pop(acc[q][ref]) + (part[r, :, lanes] + vec[4:5, lanes])
                out[r, :, lanes] = (img[1 + r, :, lanes].astype(F32) + value).astype(BF16)

        def save(r):
            for q in range(UNITS):
                part[r, :, lanes_of(q)] = pltpu.matmul_pop(acc[q][r])

        def fold(r, first, second, q):
            lanes = lanes_of(q)
            a, b = pltpu.matmul_pop(acc[q][first]), pltpu.matmul_pop(acc[q][second])
            part[r, :, lanes] += a + b
            part[r + 1, :, lanes] += a - b

        def ready(p, gath):
            lanes = lanes_of(p)
            pair = receive_stats(gath, 1 + p, vec[2:3, lanes], vec[3:4, lanes])
            return affine_of(pair, p * slabs)

        affine = ready(0, gath_a)
        here = range(slabs)
        for hook in rows_act(mid, mine, here, affine):
            hook()
        steps, last = chans_split(w_out, 0)
        contract(steps[:-TAIL])
        wait_halo(mid, 1, lanes_of(0))
        contract(steps[-TAIL:], spread(rows_act(mid, halo, here, affine), 0, TAIL))
        contract(last, spread([functools.partial(save, r) for r in middle], 2, len(last)))
        for r in outer:
            save(r)

        affine = ready(1, gath_b)
        here = range(slabs, 2 * slabs)

        def plain(r):
            return [functools.partial(activate_plain, mid, r, k, affine) for k in here]

        def pair_mix(m, a, b, sign):
            return [functools.partial(mix_rows, m, a, b, sign, k, slabs) for k in here]

        combos = [
            (1, 2, 1.0, 0, 0), (2, 1, -1.0, 1, 1), (3, 1, -1.0, None, 2),
            (3, 4, 1.0, 0, 3), (4, 3, -1.0, 1, 0), (2, 4, -1.0, None, 1),
            (0, 2, -1.0, None, 2), (5, 3, -1.0, None, 3),
        ]
        sides = {2: 2, 5: 0, 6: 0, 7: 2}

        def mixing(m):
            return pair_mix(m, *combos[m][:3])

        def product(m):
            kind, ref = combos[m][3:]

            def entry(j, q):
                columns = slice(q * SIDE, (q + 1) * SIDE)
                if kind is None:
                    tile = tile_of(w_out, sides[m], j, 1, q)
                else:
                    tile = lambda: taps[kind, j, :, columns]
                return tile, [(ref, lambda: mixed[j, m])]

            return [{q: entry(j, q) for q in range(UNITS)} for j in range(3)]

        for hook in plain(1) + plain(2) + mixing(0):
            hook()
        steps = sum((product(m) for m in range(8)), [])
        plan = spread(mixing(1) + plain(3), 0, 3)
        plan.update(spread(mixing(2) + plain(4), 3, 6))
        plan.update(spread(
            mixing(3) + [functools.partial(fold, 0, 0, 1, q) for q in range(UNITS)], 6, 10
        ))
        plan.update(spread(mixing(4) + [functools.partial(give, 1, 2)], 10, 13))
        plan.update(spread(mixing(5), 13, 15))
        contract(steps[:15], plan)
        wait_halo(mid, 2, lanes_of(1))
        plan = spread(plain(0) + mixing(6), 0, 2)
        plan.update(spread(
            plain(5) + [functools.partial(fold, 2, 3, 0, q) for q in range(UNITS)], 2, 4
        ))
        plan.update(spread(mixing(7) + [functools.partial(give, 2, 1)], 4, 7))
        plan.update({8: [functools.partial(give, 0, 2)]})
        contract(steps[15:], plan)
        give(height - 1, 3)
        all_sent(gath_in, 0)
        all_sent(gath_a, 1)
        all_sent(gath_b, 2)

    pl.run_scoped(
        body, *[pltpu.ACC(q)((width, SIDE), F32) for q in range(UNITS) for _ in range(height)]
    )


def pin(x):
    return pltpu.with_memory_space_constraint(x, pltpu.HBM)


def local(n, image, gain_in, shift_in, conv_in, gain_mid, shift_mid, conv_out, bias_out):
    height, width, chans = image.shape
    whole = pl.BlockSpec(memory_space=pltpu.HBM)
    operands = (image, gain_in[None], shift_in[None], conv_in, gain_mid[None], shift_mid[None],
                conv_out, bias_out[None])
    return pl.pallas_call(
        functools.partial(kernel, n),
        out_shape=jax.ShapeDtypeStruct(image.shape, image.dtype),
        in_specs=[whole] * len(operands),
        out_specs=pl.BlockSpec(memory_space=pltpu.VMEM),
        scratch_shapes=[
            pltpu.VMEM((height + 2, width, chans), BF16),
            pltpu.VMEM((3, height + 2, width, chans), BF16),
            pltpu.VMEM((height + 2, width, chans), BF16),
            pltpu.VMEM(conv_in.shape, BF16),
            pltpu.VMEM(conv_out.shape, BF16),
            pltpu.VMEM((2, 3, SIDE, chans), BF16),
            pltpu.VMEM((3, 8, width, SIDE), BF16),
            pltpu.VMEM((height, width, chans), F32),
            pltpu.VMEM((8, chans), F32),
            pltpu.VMEM((2, 8, chans), F32),
            pltpu.VMEM((n, LANES), F32),
            pltpu.VMEM((n, LANES), F32),
            pltpu.VMEM((n, LANES), F32),
            pltpu.SemaphoreType.DMA((height,)),
            pltpu.SemaphoreType.DMA((3,)),
            pltpu.SemaphoreType.DMA((3, 2)),
            pltpu.SemaphoreType.DMA((3, 2)),
            pltpu.SemaphoreType.DMA((3,)),
            pltpu.SemaphoreType.DMA((3,)),
        ],
        compiler_params=pltpu.CompilerParams(
            collective_id=0, has_side_effects=True, vmem_limit_bytes=44 * 1024 * 1024
        ),
    )(*[pin(x) for x in operands])


def solution(mesh):
    n = mesh.shape["rows"]
    in_specs = (P(("img", "rows"), None, None), P(), P(), P(), P(), P(), P(), P())
    out_specs = P(("img", "rows"), None, None)
    return jax.shard_map(
        functools.partial(local, n), mesh=mesh, in_specs=in_specs, out_specs=out_specs,
        check_vma=False,
    )
```

```python
import functools

import jax
import jax.numpy as jnp
from jax import lax
from jax.experimental import pallas as pl
from jax.experimental.pallas import tpu as pltpu
from jax.sharding import PartitionSpec as P

GROUPS = 32
LANES = 128
SIDE = 256
UNITS = 2
CHUNK = 32
PAD = 8
LEAD = 4
SOAK = 1
DRAIN = 2
MESH = pl.DeviceIdType.MESH
BF16, F32 = jnp.bfloat16, jnp.float32


def packed(sums, squares):
    chans = sums.shape[1]
    pieces = [part[:, k : k + LANES] for part in (sums, squares) for k in range(0, chans, LANES)]
    return jnp.concatenate(pieces, axis=0)


def flat(tile):
    return jnp.concatenate([tile[k : k + 1] for k in range(tile.shape[0])], axis=1)


def group_total(tile, size):
    lane = lax.broadcasted_iota(jnp.int32, tile.shape, 1)
    step = 1
    while step < size:
        far = min(4, size // step)
        place = (lane // step) % far
        turned = {d: pltpu.roll(tile, (d * step) % LANES, 1) for d in range(1 - far, far) if d}
        total = tile
        for p in range(1, far):
            other = turned[p]
            for d in range(p):
                other = jnp.where(place == d, turned[p - far], other)
            total = total + other
        tile = total
        step *= far
    return tile


def kernel(n, image, gain_in, shift_in, conv_in, gain_mid, shift_mid, conv_out, bias_out, out,
           img, act, mid, w_in, w_out, taps, mixed, part, vec, sums, gath_in, gath_a, gath_b,
           img_sem, load_sem, halo_send, halo_recv, stat_send, stat_recv):
    me = lax.axis_index("rows")
    height, width, chans = image.shape
    size = chans // GROUPS
    count = float(height * width * size * n)
    parts = chans // LANES
    depth = chans // SIDE
    slabs = SIDE // LANES
    share = height // UNITS

    order = [0, height - 1] + list(range(1, height - 1))
    loads = {
        r: pltpu.make_async_copy(image.at[r], img.at[1 + r], img_sem.at[r]) for r in order
    }
    for r in order:
        loads[r].start()
    load_w_in = pltpu.make_async_copy(conv_in, w_in, load_sem.at[0])
    load_w_out = pltpu.make_async_copy(conv_out, w_out, load_sem.at[1])

    barrier = pltpu.get_barrier_semaphore()
    for d in range(1, n):
        pl.semaphore_signal(
            barrier, inc=1, device_id={"rows": lax.rem(me + d, n)}, device_id_type=MESH
        )

    def add_stats(value, lanes):
        folded = value.reshape(value.shape[0] // 8, 8, value.shape[1])
        sums[0, :, lanes] += jnp.sum(folded, axis=0)
        sums[1, :, lanes] += jnp.sum(folded * folded, axis=0)

    def stat_copy(gath, which, d):
        return pltpu.make_async_remote_copy(
            src_ref=gath.at[pl.ds(0, 1)],
            dst_ref=gath.at[pl.ds(d, 1)],
            send_sem=stat_send.at[which],
            recv_sem=stat_recv.at[which],
            device_id={"rows": lax.rem(me + d, n)},
            device_id_type=MESH,
        )

    def prepare_stats(gath, lanes):
        tile = packed(
            jnp.sum(sums[0, :, lanes], axis=0, keepdims=True),
            jnp.sum(sums[1, :, lanes], axis=0, keepdims=True),
        )
        tile = group_total(tile, size)
        lane = lax.broadcasted_iota(jnp.int32, tile.shape, 1)
        row = lax.broadcasted_iota(jnp.int32, tile.shape, 0)
        mine = jnp.where(lax.rem(lane, size) == row, tile, 0.0)
        gath[0:1] = jnp.sum(mine, axis=0, keepdims=True)

    def send_stats(gath, which):
        for d in range(1, n):
            stat_copy(gath, which, d).start()

    def all_sent(gath, which):
        pltpu.make_async_copy(
            gath.at[pl.ds(1, n - 1)], gath.at[pl.ds(1, n - 1)], stat_send.at[which]
        ).wait()

    def receive_stats(gath, which, gain, shift):
        pltpu.make_async_copy(
            gath.at[pl.ds(1, n - 1)], gath.at[pl.ds(1, n - 1)], stat_recv.at[which]
        ).wait()
        pieces = gain.shape[1] // LANES
        total = jnp.sum(gath[...], axis=0, keepdims=True) / count
        total = jnp.broadcast_to(total, (2 * pieces, LANES))
        lane = lax.broadcasted_iota(jnp.int32, total.shape, 1)
        row = lax.broadcasted_iota(jnp.int32, total.shape, 0)
        tile = jnp.take_along_axis(total, lane - lax.rem(lane, size) + row, axis=1)
        mean, square = tile[:pieces], tile[pieces:]
        variance = jnp.maximum(square - mean * mean, 0.0)
        scale = flat(lax.rsqrt(variance + 1e-06)) * (0.5 * gain)
        return scale, 0.5 * shift - flat(mean) * scale

    def halo_copies(buf, which, lanes):
        up = pltpu.make_async_remote_copy(
            src_ref=buf.at[1, :, lanes],
            dst_ref=buf.at[height + 1, :, lanes],
            send_sem=halo_send.at[which, 0],
            recv_sem=halo_recv.at[which, 0],
            device_id={"rows": jnp.maximum(me - 1, 0)},
            device_id_type=MESH,
        )
        down = pltpu.make_async_remote_copy(
            src_ref=buf.at[height, :, lanes],
            dst_ref=buf.at[0, :, lanes],
            send_sem=halo_send.at[which, 1],
            recv_sem=halo_recv.at[which, 1],
            device_id={"rows": jnp.minimum(me + 1, n - 1)},
            device_id_type=MESH,
        )
        return up, down

    def send_halo(buf, which, lanes):
        up, down = halo_copies(buf, which, lanes)

        @pl.when(me > 0)
        def _():
            up.start()

        @pl.when(me < n - 1)
        def _():
            down.start()

    def wait_halo(buf, which, lanes):
        up, down = halo_copies(buf, which, lanes)

        @pl.when(me > 0)
        def _():
            up.wait_send()
            down.wait_recv()

        @pl.when(me < n - 1)
        def _():
            down.wait_send()
            up.wait_recv()

    def activated(buf, row, k, affine):
        lanes = slice(k * LANES, (k + 1) * LANES)
        scale, shift = affine[k]
        half = buf[row, :, lanes].astype(F32) * scale + shift
        value = half + half * jnp.tanh(half)
        if row == 0:
            value = jnp.where(me > 0, value, 0.0)
        if row == height + 1:
            value = jnp.where(me < n - 1, value, 0.0)
        return value

    inside = pl.ds(PAD, width)

    def activate(buf, row, k, affine):
        act[row, k, inside] = activated(buf, row, k, affine)

    def activate_round(buf, row, k, affine):
        act[row, k, inside] = activated(buf, row, k, affine).astype(BF16).astype(F32)

    def mix_rows(m, a, b, sign, k, base):
        mixed[m, k - base, inside] = act[a, k, inside] + sign * act[b, k, inside]

    def shifted(buf, row, j, k):
        cols = pl.ds(PAD + j - 1, width)
        return jnp.concatenate(
            [buf[row, k * slabs + m, cols] for m in range(slabs)], axis=1
        )

    def mix_taps(p):
        def step(t, _):
            rows = pl.ds(pl.multiple_of(t * CHUNK, CHUNK), CHUNK)
            source = pl.ds(pl.multiple_of(p * SIDE + t * CHUNK, CHUNK), CHUNK)
            for j in range(3):
                ends = 0.5 * (
                    w_out[0, j, source].astype(F32) + w_out[2, j, source].astype(F32)
                )
                centre = 0.5 * w_out[1, j, source].astype(F32)
                taps[p, 0, j, rows] = (ends + centre).astype(BF16)
                taps[p, 1, j, rows] = (ends - centre).astype(BF16)
            return 0

        lax.fori_loop(0, SIDE // CHUNK, step, 0)

    def body(*accs):
        acc = [accs[q * height : (q + 1) * height] for q in range(UNITS)]

        zero = jnp.zeros((SIDE, SIDE), BF16)
        for q in range(UNITS):
            for s in range(2):
                pltpu.matmul_acc_lhs(acc[q][0], zero, load_staged_rhs=s)
        for q in range(UNITS):
            for r in range(height):
                pltpu.matmul_pop(acc[q][r])

        def contract(steps, hooks=None):
            def push(t):
                for q, (tile, _) in steps[t].items():
                    pltpu.matmul_push_rhs(tile(), staging_register=t % 2, mxu_index=q)

            push(0)
            for t, step in enumerate(steps):
                if t + 1 < len(steps):
                    push(t + 1)
                for hook in (hooks or {}).get(t, []):
                    hook()
                for m in range(height):
                    for q, (_, pairs) in step.items():
                        if m < len(pairs):
                            ref, left = pairs[m]
                            pltpu.matmul_acc_lhs(
                                acc[q][ref], left(), load_staged_rhs=t % 2 if m == 0 else None
                            )

        def tile_of(weights, i, j, k, p):
            return lambda: weights[
                i, j, k * SIDE : (k + 1) * SIDE, p * SIDE : (p + 1) * SIDE
            ]

        def left_of(j, row, k):
            return lambda: shifted(act, row, j, k)

        spots = [(i, j) for j in range(3) for i in (1, 0, 2)]

        def inner(i, rows):
            return [r for r in rows if 1 <= r + i <= height]

        def place(p, r):
            return r // share, p * share + r % share

        def rows_split(w, p, k):
            def entry(i, j, q):
                rows = inner(i, range(q * share, (q + 1) * share))
                pairs = [(place(p, r)[1], left_of(j, r + i, k)) for r in rows]
                return tile_of(w, i, j, k, p), pairs

            own = [{q: entry(i, j, q) for q in range(UNITS)} for i, j in spots]
            ends = [
                {
                    q: (tile_of(w, i, j, k, p), [(place(p, r)[1], left_of(j, r + i, k))])
                    for q, i, r in ((0, 0, 0), (UNITS - 1, 2, height - 1))
                }
                for j in range(3)
            ]
            return own, ends

        def rows_first(w, p, k):
            queues = []
            for q in range(UNITS):
                rows = list(range(q * share, (q + 1) * share))
                inputs = range(1, height + 1) if q == 0 else range(height, 0, -1)
                queues.append([
                    (tile_of(w, x - r, j, k, p), [(place(p, r)[1], left_of(j, x, k))])
                    for x in inputs
                    for j in range(3)
                    for r in (rows if q == 0 else rows[::-1])
                    if 0 <= x - r <= 2
                ])
            return [dict(enumerate(step)) for step in zip(*queues, strict=True)]

        def spread(hooks, first, last):
            assert first < last
            steps = range(first, last)
            plan = {t: [] for t in steps}
            for m, hook in enumerate(hooks):
                plan[first + m * len(steps) // len(hooks)].append(hook)
            return plan

        def lanes_of(p):
            return slice(p * SIDE, (p + 1) * SIDE)

        def rows_act(buf, rows, ks, affine):
            return [
                functools.partial(activate, buf, r, k, affine) for k in ks for r in rows
            ]

        def affine_of(pair, first=0):
            scale, shift = pair
            return {
                first + k: (scale[:, k * LANES : (k + 1) * LANES], shift[:, k * LANES : (k + 1) * LANES])
                for k in range(scale.shape[1] // LANES)
            }

        mine = range(1, height + 1)
        halo = (0, height + 1)

        sums[...] = jnp.zeros_like(sums)
        for buf in (act, mixed):
            edge = jnp.zeros(buf.shape[:2] + (PAD, LANES), F32)
            buf[:, :, 0:PAD] = edge
            buf[:, :, PAD + width : 2 * PAD + width] = edge

        def stats_step(r, k, _):
            cols = pl.ds(pl.multiple_of(k * CHUNK, CHUNK), CHUNK)
            add_stats(img[1 + r, cols].astype(F32), slice(None))
            return 0

        for r in order:
            loads[r].wait()
            if r == order[-1]:
                for k, source in enumerate((gain_in, shift_in, gain_mid, shift_mid, bias_out)):
                    pltpu.make_async_copy(source, vec.at[pl.ds(k, 1)], load_sem.at[2]).start()
                load_w_in.start()
                load_w_out.start()
            lax.fori_loop(0, width // CHUNK, functools.partial(stats_step, r), 0)
        prepare_stats(gath_in, slice(None))
        pl.semaphore_wait(barrier, n - 1)
        send_stats(gath_in, 0)
        send_halo(img, 0, slice(None))
        sums[...] = jnp.zeros_like(sums)
        load_w_in.wait()
        load_w_out.wait()
        for p in range(depth):
            mix_taps(p)
        pltpu.make_async_copy(vec.at[pl.ds(0, 5)], vec.at[pl.ds(0, 5)], load_sem.at[2]).wait()
        affine = affine_of(receive_stats(gath_in, 0, vec[0:1], vec[1:2]))

        def keep(p, r):
            lanes = lanes_of(p)
            q, ref = place(p, r)
            value = pltpu.matmul_pop(acc[q][ref]).astype(BF16)
            mid[1 + r, :, lanes] = value
            add_stats(value.astype(F32), lanes)

        middle = range(1, height - 1)
        outer = (0, height - 1)

        def kept(p, rows):
            return [functools.partial(keep, p, r) for r in rows]

        def both(p):
            first = [rows_split(w_in, p, k) for k in range(depth)]
            return [sum((pair[m] for pair in first), []) for m in range(2)]

        own_b, ends_b = both(1)
        _, ends_a = both(0)
        near = (1, height)
        far = [r for r in mine if r not in near]
        for hook in rows_act(img, near, range(slabs), affine):
            hook()
        start = rows_first(w_in, 0, 0)
        plan = spread(rows_act(img, far, range(slabs), affine), 0, 4)
        plan.update(spread(rows_act(img, mine, range(slabs, parts), affine), 4, len(start)))
        contract(start, plan)
        later = sum((rows_split(w_in, 0, k)[0] for k in range(1, depth)), [])
        contract(later)
        contract(own_b[:LEAD])
        wait_halo(img, 0, slice(None))
        contract(
            own_b[LEAD : LEAD + SOAK],
            spread(rows_act(img, halo, range(slabs), affine), 0, SOAK),
        )
        plan = spread(rows_act(img, halo, range(slabs, parts), affine), 0, 2)
        plan.update(spread(kept(0, middle), 3, len(ends_a)))
        contract(ends_a, plan)
        contract(
            own_b[LEAD + SOAK : LEAD + SOAK + DRAIN],
            spread(
                kept(0, outer) + [functools.partial(prepare_stats, gath_a, lanes_of(0))], 0, DRAIN
            ),
        )
        send_stats(gath_a, 1)
        send_halo(mid, 1, lanes_of(0))
        contract(own_b[LEAD + SOAK + DRAIN :])
        contract(ends_b, spread(kept(1, middle), 1, len(ends_b)))
        for hook in kept(1, outer):
            hook()
        prepare_stats(gath_b, lanes_of(1))
        send_stats(gath_b, 2)
        send_halo(mid, 2, lanes_of(1))

        def give(r, ref):
            for q in range(UNITS):
                lanes = lanes_of(q)
                value = pltpu.matmul_pop(acc[q][ref]) + (part[r, :, lanes] + vec[4:5, lanes])
                out[r, :, lanes] = (img[1 + r, :, lanes].astype(F32) + value).astype(BF16)

        def fold(p, r, first, second, q):
            lanes = lanes_of(q)
            a, b = pltpu.matmul_pop(acc[q][first]), pltpu.matmul_pop(acc[q][second])
            if p == 0:
                part[r, :, lanes] = a + b
                part[r + 1, :, lanes] = a - b
            else:
                part[r, :, lanes] += a + b
                part[r + 1, :, lanes] += a - b

        def save(r, ref):
            for q in range(UNITS):
                part[r, :, lanes_of(q)] += pltpu.matmul_pop(acc[q][ref])

        combos = [
            (1, 2, 1.0, 0, 0), (2, 1, -1.0, 1, 1), (3, 1, -1.0, None, 2),
            (3, 4, 1.0, 0, 3), (4, 3, -1.0, 1, 0), (2, 4, -1.0, None, 1),
            (0, 2, -1.0, None, 2), (5, 3, -1.0, None, 3),
        ]
        sides = {2: 2, 5: 0, 6: 0, 7: 2}

        def product(m, p):
            kind, ref = combos[m][3:]

            def entry(j, q):
                columns = slice(q * SIDE, (q + 1) * SIDE)
                if kind is None:
                    tile = tile_of(w_out, sides[m], j, p, q)
                else:
                    tile = lambda: taps[p, kind, j, :, columns]
                return tile, [(ref, lambda: shifted(mixed, m, j, 0))]

            return [{q: entry(j, q) for q in range(UNITS)} for j in range(3)]

        def second(p, affine):
            here = range(p * slabs, (p + 1) * slabs)
            put = save if p < depth - 1 else give

            def plain(r):
                return [functools.partial(activate_round, mid, r, k, affine) for k in here]

            def mixing(m):
                return [
                    functools.partial(mix_rows, m, *combos[m][:3], k, p * slabs) for k in here
                ]

            def folding(r, first, other):
                return [functools.partial(fold, p, r, first, other, q) for q in range(UNITS)]

            steps = sum((product(m, p) for m in range(8)), [])
            early = spread(mixing(1) + plain(3), 0, 3)
            early.update(spread(mixing(2) + plain(4), 3, 6))
            early.update(spread(mixing(3) + folding(0, 0, 1), 6, 10))
            early.update(spread(mixing(4) + [functools.partial(put, 1, 2)], 10, 13))
            early.update(spread(mixing(5), 13, 15))
            late = spread(plain(0) + mixing(6), 0, 2)
            late.update(spread(plain(5) + folding(2, 3, 0), 2, 4))
            late.update(spread(mixing(7) + [functools.partial(put, 2, 1)], 4, 7))
            late.update({8: [functools.partial(put, 0, 2)]})
            opening = plain(1) + plain(2) + mixing(0)
            return opening, steps[:15], early, steps[15:], late, functools.partial(put, height - 1, 3)

        def ready(p, gath):
            lanes = lanes_of(p)
            pair = receive_stats(gath, 1 + p, vec[2:3, lanes], vec[3:4, lanes])
            return second(p, affine_of(pair, p * slabs))

        opening, steps, plan, rest, rest_plan, closing = ready(0, gath_a)
        for hook in opening:
            hook()
        contract(steps, plan)
        wait_halo(mid, 1, lanes_of(0))
        contract(rest, rest_plan)
        opening, steps, plan, last, last_plan, final = ready(1, gath_b)
        for hook in opening:
            hook()
        plan[2] = plan[2] + [closing]
        contract(steps, plan)
        wait_halo(mid, 2, lanes_of(1))
        contract(last, last_plan)
        final()
        all_sent(gath_in, 0)
        all_sent(gath_a, 1)
        all_sent(gath_b, 2)

    pl.run_scoped(
        body, *[pltpu.ACC(q)((width, SIDE), F32) for q in range(UNITS) for _ in range(height)]
    )


def pin(x):
    return pltpu.with_memory_space_constraint(x, pltpu.HBM)


def local(n, image, gain_in, shift_in, conv_in, gain_mid, shift_mid, conv_out, bias_out):
    height, width, chans = image.shape
    whole = pl.BlockSpec(memory_space=pltpu.HBM)
    operands = (image, gain_in[None], shift_in[None], conv_in, gain_mid[None], shift_mid[None],
                conv_out, bias_out[None])
    return pl.pallas_call(
        functools.partial(kernel, n),
        out_shape=jax.ShapeDtypeStruct(image.shape, image.dtype),
        in_specs=[whole] * len(operands),
        out_specs=pl.BlockSpec(memory_space=pltpu.VMEM),
        scratch_shapes=[
            pltpu.VMEM((height + 2, width, chans), BF16),
            pltpu.VMEM((height + 2, chans // LANES, width + 2 * PAD, LANES), F32),
            pltpu.VMEM((height + 2, width, chans), BF16),
            pltpu.VMEM(conv_in.shape, BF16),
            pltpu.VMEM(conv_out.shape, BF16),
            pltpu.VMEM((chans // SIDE, 2, 3, SIDE, chans), BF16),
            pltpu.VMEM((8, SIDE // LANES, width + 2 * PAD, LANES), F32),
            pltpu.VMEM((height, width, chans), F32),
            pltpu.VMEM((8, chans), F32),
            pltpu.VMEM((2, 8, chans), F32),
            pltpu.VMEM((n, LANES), F32),
            pltpu.VMEM((n, LANES), F32),
            pltpu.VMEM((n, LANES), F32),
            pltpu.SemaphoreType.DMA((height,)),
            pltpu.SemaphoreType.DMA((3,)),
            pltpu.SemaphoreType.DMA((3, 2)),
            pltpu.SemaphoreType.DMA((3, 2)),
            pltpu.SemaphoreType.DMA((3,)),
            pltpu.SemaphoreType.DMA((3,)),
        ],
        compiler_params=pltpu.CompilerParams(
            collective_id=0, has_side_effects=True, vmem_limit_bytes=44 * 1024 * 1024
        ),
    )(*[pin(x) for x in operands])


def solution(mesh):
    n = mesh.shape["rows"]
    in_specs = (P(("img", "rows"), None, None), P(), P(), P(), P(), P(), P(), P())
    out_specs = P(("img", "rows"), None, None)
    return jax.shard_map(
        functools.partial(local, n), mesh=mesh, in_specs=in_specs, out_specs=out_specs,
        check_vma=False,
    )
```

```python
import functools

import jax
import jax.numpy as jnp
from jax import lax
from jax.experimental import pallas as pl
from jax.experimental.pallas import tpu as pltpu
from jax.sharding import PartitionSpec as P

GROUPS = 32
LANES = 128
SIDE = 256
UNITS = 2
CHUNK = 32
PAD = 8
LEAD = 1
TURN = 5
SOAK = 1
DRAIN = 3
MESH = pl.DeviceIdType.MESH
BF16, F32 = jnp.bfloat16, jnp.float32


def packed(sums, squares):
    chans = sums.shape[1]
    pieces = [part[:, k : k + LANES] for part in (sums, squares) for k in range(0, chans, LANES)]
    return jnp.concatenate(pieces, axis=0)


def flat(tile):
    return jnp.concatenate([tile[k : k + 1] for k in range(tile.shape[0])], axis=1)


def group_total(tile, size):
    lane = lax.broadcasted_iota(jnp.int32, tile.shape, 1)
    step = 1
    while step < size:
        far = min(4, size // step)
        place = (lane // step) % far
        turned = {d: pltpu.roll(tile, (d * step) % LANES, 1) for d in range(1 - far, far) if d}
        total = tile
        for p in range(1, far):
            other = turned[p]
            for d in range(p):
                other = jnp.where(place == d, turned[p - far], other)
            total = total + other
        tile = total
        step *= far
    return tile


def kernel(n, image, gain_in, shift_in, conv_in, gain_mid, shift_mid, conv_out, bias_out, out,
           img, act, mid, w_in, w_out, taps_in, taps, mixed, part, vec, sums, gath_in, gath_a, gath_b,
           img_sem, load_sem, halo_send, halo_recv, stat_send, stat_recv):
    me = lax.axis_index("rows")
    height, width, chans = image.shape
    size = chans // GROUPS
    count = float(height * width * size * n)
    parts = chans // LANES
    depth = chans // SIDE
    slabs = SIDE // LANES
    share = height // UNITS

    order = [0, height - 1] + list(range(1, height - 1))
    loads = {
        r: pltpu.make_async_copy(image.at[r], img.at[1 + r], img_sem.at[r]) for r in order
    }
    for r in order:
        loads[r].start()
    load_w_in = pltpu.make_async_copy(conv_in, w_in, load_sem.at[0])
    load_w_out = pltpu.make_async_copy(conv_out, w_out, load_sem.at[1])

    barrier = pltpu.get_barrier_semaphore()
    for d in range(1, n):
        pl.semaphore_signal(
            barrier, inc=1, device_id={"rows": lax.rem(me + d, n)}, device_id_type=MESH
        )

    def add_stats(value, lanes):
        folded = value.reshape(value.shape[0] // 8, 8, value.shape[1])
        sums[0, :, lanes] += jnp.sum(folded, axis=0)
        sums[1, :, lanes] += jnp.sum(folded * folded, axis=0)

    def stat_copy(gath, which, d):
        return pltpu.make_async_remote_copy(
            src_ref=gath.at[pl.ds(0, 1)],
            dst_ref=gath.at[pl.ds(d, 1)],
            send_sem=stat_send.at[which],
            recv_sem=stat_recv.at[which],
            device_id={"rows": lax.rem(me + d, n)},
            device_id_type=MESH,
        )

    def prepare_stats(gath, lanes):
        tile = packed(
            jnp.sum(sums[0, :, lanes], axis=0, keepdims=True),
            jnp.sum(sums[1, :, lanes], axis=0, keepdims=True),
        )
        tile = group_total(tile, size)
        lane = lax.broadcasted_iota(jnp.int32, tile.shape, 1)
        row = lax.broadcasted_iota(jnp.int32, tile.shape, 0)
        mine = jnp.where(lax.rem(lane, size) == row, tile, 0.0)
        gath[0:1] = jnp.sum(mine, axis=0, keepdims=True)

    def send_stats(gath, which):
        for d in sorted(range(1, n), key=lambda d: min(d, n - d)):
            stat_copy(gath, which, d).start()

    def all_sent(gath, which):
        pltpu.make_async_copy(
            gath.at[pl.ds(1, n - 1)], gath.at[pl.ds(1, n - 1)], stat_send.at[which]
        ).wait()

    def receive_stats(gath, which, gain, shift):
        pltpu.make_async_copy(
            gath.at[pl.ds(1, n - 1)], gath.at[pl.ds(1, n - 1)], stat_recv.at[which]
        ).wait()
        pieces = gain.shape[1] // LANES
        total = jnp.sum(gath[...], axis=0, keepdims=True) * (1.0 / count)
        total = jnp.broadcast_to(total, (2 * pieces, LANES))
        lane = lax.broadcasted_iota(jnp.int32, total.shape, 1)
        row = lax.broadcasted_iota(jnp.int32, total.shape, 0)
        tile = jnp.take_along_axis(total, lane - lax.rem(lane, size) + row, axis=1)
        mean, square = tile[:pieces], tile[pieces:]
        variance = jnp.maximum(square - mean * mean, 0.0)
        scale = flat(lax.rsqrt(variance + 1e-06)) * (0.5 * gain)
        return scale, 0.5 * shift - flat(mean) * scale

    def halo_copies(buf, which, lanes):
        up = pltpu.make_async_remote_copy(
            src_ref=buf.at[1, :, lanes],
            dst_ref=buf.at[height + 1, :, lanes],
            send_sem=halo_send.at[which, 0],
            recv_sem=halo_recv.at[which, 0],
            device_id={"rows": jnp.maximum(me - 1, 0)},
            device_id_type=MESH,
        )
        down = pltpu.make_async_remote_copy(
            src_ref=buf.at[height, :, lanes],
            dst_ref=buf.at[0, :, lanes],
            send_sem=halo_send.at[which, 1],
            recv_sem=halo_recv.at[which, 1],
            device_id={"rows": jnp.minimum(me + 1, n - 1)},
            device_id_type=MESH,
        )
        return up, down

    def send_halo(buf, which, lanes):
        up, down = halo_copies(buf, which, lanes)

        @pl.when(me > 0)
        def _():
            up.start()

        @pl.when(me < n - 1)
        def _():
            down.start()

    def wait_halo(buf, which, lanes):
        up, down = halo_copies(buf, which, lanes)

        @pl.when(me > 0)
        def _():
            up.wait_send()
            down.wait_recv()

        @pl.when(me < n - 1)
        def _():
            down.wait_send()
            up.wait_recv()

    def activated(buf, row, k, affine):
        lanes = slice(k * LANES, (k + 1) * LANES)
        scale, shift = affine[k]
        half = buf[row, :, lanes].astype(F32) * scale + shift
        value = half + half * jnp.tanh(half)
        if row == 0:
            value = jnp.where(me > 0, value, 0.0)
        if row == height + 1:
            value = jnp.where(me < n - 1, value, 0.0)
        return value

    inside = pl.ds(PAD, width)

    def activate(buf, row, k, affine):
        act[row, k, inside] = activated(buf, row, k, affine)

    def activate_round(buf, row, k, affine):
        act[row, k, inside] = activated(buf, row, k, affine).astype(BF16).astype(F32)

    def mix_rows(m, a, b, sign, k, base):
        mixed[m, k - base, inside] = act[a, k, inside] + sign * act[b, k, inside]

    def mix_rounded(m, a, b, sign, k):
        first = act[a, k, inside].astype(BF16).astype(F32)
        mixed[m, k, inside] = first + sign * act[b, k, inside].astype(BF16).astype(F32)

    def shifted(buf, row, j, k):
        cols = pl.ds(PAD + j - 1, width)
        return jnp.concatenate(
            [buf[row, k * slabs + m, cols] for m in range(slabs)], axis=1
        )

    def mix_taps_in(columns):
        def step(t, _):
            rows = pl.ds(pl.multiple_of(t * CHUNK, CHUNK), CHUNK)
            for j in range(3):
                ends = 0.5 * (
                    w_in[0, j, rows, columns].astype(F32) + w_in[2, j, rows, columns].astype(F32)
                )
                centre = 0.5 * w_in[1, j, rows, columns].astype(F32)
                taps_in[0, j, rows] = (ends + centre).astype(BF16)
                taps_in[1, j, rows] = (ends - centre).astype(BF16)
            return 0

        lax.fori_loop(0, chans // CHUNK, step, 0)

    def mix_taps(p):
        def step(t, _):
            rows = pl.ds(pl.multiple_of(t * CHUNK, CHUNK), CHUNK)
            source = pl.ds(pl.multiple_of(p * SIDE + t * CHUNK, CHUNK), CHUNK)
            for j in range(3):
                ends = 0.5 * (
                    w_out[0, j, source].astype(F32) + w_out[2, j, source].astype(F32)
                )
                centre = 0.5 * w_out[1, j, source].astype(F32)
                taps[p, 0, j, rows] = (ends + centre).astype(BF16)
                taps[p, 1, j, rows] = (ends - centre).astype(BF16)
            return 0

        lax.fori_loop(0, SIDE // CHUNK, step, 0)

    def body(*accs):
        acc = [accs[q * height : (q + 1) * height] for q in range(UNITS)]

        zero = jnp.zeros((SIDE, SIDE), BF16)
        for q in range(UNITS):
            for s in range(2):
                pltpu.matmul_acc_lhs(acc[q][0], zero, load_staged_rhs=s)
        for q in range(UNITS):
            for r in range(height):
                pltpu.matmul_pop(acc[q][r])

        def contract(steps, hooks=None):
            def push(t):
                for q, (tile, _) in steps[t].items():
                    pltpu.matmul_push_rhs(tile(), staging_register=t % 2, mxu_index=q)

            push(0)
            for t, step in enumerate(steps):
                if t + 1 < len(steps):
                    push(t + 1)
                for hook in (hooks or {}).get(t, []):
                    hook()
                for m in range(height):
                    for q, (_, pairs) in step.items():
                        if m < len(pairs):
                            ref, left = pairs[m]
                            pltpu.matmul_acc_lhs(
                                acc[q][ref], left(), load_staged_rhs=t % 2 if m == 0 else None
                            )

        def tile_of(weights, i, j, k, p):
            return lambda: weights[
                i, j, k * SIDE : (k + 1) * SIDE, p * SIDE : (p + 1) * SIDE
            ]

        def left_of(j, row, k):
            return lambda: shifted(act, row, j, k)

        spots = [(i, j) for j in range(3) for i in (1, 0, 2)]

        def inner(i, rows):
            return [r for r in rows if 1 <= r + i <= height]

        def place(p, r):
            return r // share, p * share + r % share

        def rows_split(w, p, k):
            def entry(i, j, q):
                rows = inner(i, range(q * share, (q + 1) * share))
                pairs = [(place(p, r)[1], left_of(j, r + i, k)) for r in rows]
                return tile_of(w, i, j, k, p), pairs

            own = [{q: entry(i, j, q) for q in range(UNITS)} for i, j in spots]
            ends = [
                {
                    q: (tile_of(w, i, j, k, p), [(place(p, r)[1], left_of(j, r + i, k))])
                    for q, i, r in ((0, 0, 0), (UNITS - 1, 2, height - 1))
                }
                for j in range(3)
            ]
            return own, ends

        def rows_first(w, p, k):
            queues = []
            for q in range(UNITS):
                rows = list(range(q * share, (q + 1) * share))
                inputs = range(1, height + 1) if q == 0 else range(height, 0, -1)
                queues.append([
                    (tile_of(w, x - r, j, k, p), [(place(p, r)[1], left_of(j, x, k))])
                    for x in inputs
                    for j in range(3)
                    for r in (rows if q == 0 else rows[::-1])
                    if 0 <= x - r <= 2
                ])
            return [dict(enumerate(step)) for step in zip(*queues, strict=True)]

        def spread(hooks, first, last):
            assert first < last
            steps = range(first, last)
            plan = {t: [] for t in steps}
            for m, hook in enumerate(hooks):
                plan[first + m * len(steps) // len(hooks)].append(hook)
            return plan

        def lanes_of(p):
            return slice(p * SIDE, (p + 1) * SIDE)

        def rows_act(buf, rows, ks, affine):
            return [
                functools.partial(activate, buf, r, k, affine) for k in ks for r in rows
            ]

        def affine_of(pair, first=0):
            scale, shift = pair
            return {
                first + k: (scale[:, k * LANES : (k + 1) * LANES], shift[:, k * LANES : (k + 1) * LANES])
                for k in range(scale.shape[1] // LANES)
            }

        mine = range(1, height + 1)
        halo = (0, height + 1)

        sums[...] = jnp.zeros_like(sums)
        for buf in (act, mixed):
            edge = jnp.zeros(buf.shape[:2] + (PAD, LANES), F32)
            buf[:, :, 0:PAD] = edge
            buf[:, :, PAD + width : 2 * PAD + width] = edge

        def stats_step(r, k, _):
            cols = pl.ds(pl.multiple_of(k * CHUNK, CHUNK), CHUNK)
            add_stats(img[1 + r, cols].astype(F32), slice(None))
            return 0

        for r in order:
            loads[r].wait()
            if r == order[-1]:
                for k, source in enumerate((gain_in, shift_in, gain_mid, shift_mid, bias_out)):
                    pltpu.make_async_copy(source, vec.at[pl.ds(k, 1)], load_sem.at[2]).start()
                load_w_in.start()
                load_w_out.start()
            lax.fori_loop(0, width // CHUNK, functools.partial(stats_step, r), 0)
        prepare_stats(gath_in, slice(None))
        pl.semaphore_wait(barrier, n - 1)
        send_stats(gath_in, 0)
        send_halo(img, 0, slice(None))
        sums[...] = jnp.zeros_like(sums)
        load_w_in.wait()
        mix_taps_in(slice(SIDE, 2 * SIDE))
        load_w_out.wait()
        for p in range(depth):
            mix_taps(p)
        pltpu.make_async_copy(vec.at[pl.ds(0, 5)], vec.at[pl.ds(0, 5)], load_sem.at[2]).wait()
        affine = affine_of(receive_stats(gath_in, 0, vec[0:1], vec[1:2]))

        def keep(p, r):
            lanes = lanes_of(p)
            q, ref = place(p, r)
            value = pltpu.matmul_pop(acc[q][ref]).astype(BF16)
            mid[1 + r, :, lanes] = value
            add_stats(value.astype(F32), lanes)

        middle = range(1, height - 1)
        outer = (0, height - 1)

        def kept(p, rows):
            return [functools.partial(keep, p, r) for r in rows]

        def both(p):
            first = [rows_split(w_in, p, k) for k in range(depth)]
            return [sum((pair[m] for pair in first), []) for m in range(2)]

        combos = [
            (1, 2, 1.0, 0, 0), (2, 1, -1.0, 1, 1), (3, 1, -1.0, None, 2),
            (3, 4, 1.0, 0, 3), (4, 3, -1.0, 1, 0), (2, 4, -1.0, None, 1),
            (0, 2, -1.0, None, 2), (5, 3, -1.0, None, 3),
        ]
        sides = {2: 2, 5: 0, 6: 0, 7: 2}

        _, ends_a = both(0)
        pairs = ((0, 1, 2, 6), (3, 4, 5, 7))

        def wide(stage):
            ref = (stage + share) % height

            def entry(j, k, q):
                m = pairs[q][stage]
                kind = combos[m][3]
                if kind is None:
                    tile = tile_of(w_in, sides[m], j, k, 1)
                else:
                    tile = lambda: taps_in[kind, j, k * SIDE : (k + 1) * SIDE]
                return tile, [(ref, lambda: shifted(mixed, m, j, k))]

            return [
                {q: entry(j, k, q) for q in range(UNITS)} for k in range(depth) for j in range(3)
            ]

        def mixing_in(stage):
            return [
                functools.partial(mix_rounded, pairs[q][stage], *combos[pairs[q][stage]][:3], k)
                for k in range(parts) for q in range(UNITS)
            ]

        def split_b(q):
            lanes = lanes_of(1)
            a, b = pltpu.matmul_pop(acc[q][share]), pltpu.matmul_pop(acc[q][share + 1])
            part[share * q, :, lanes] = a + b
            part[share * q + 1, :, lanes] = a - b

        def finish_b(q, r, ref):
            lanes = lanes_of(1)
            value = (part[r, :, lanes] + pltpu.matmul_pop(acc[q][ref])).astype(BF16)
            mid[1 + r, :, lanes] = value
            add_stats(value.astype(F32), lanes)

        near = (1, height)
        far = [r for r in mine if r not in near]
        for hook in rows_act(img, near, range(slabs), affine):
            hook()
        start = rows_first(w_in, 0, 0)
        plan = spread(rows_act(img, far, range(slabs), affine), 0, 4)
        plan.update(spread(rows_act(img, mine, range(slabs, parts), affine), 4, len(start)))
        contract(start, plan)
        later = sum((rows_split(w_in, 0, k)[0] for k in range(1, depth)), [])
        plan = spread(mixing_in(0), 0, 5)
        plan.update(spread(mixing_in(1), 5, len(later)))
        contract(later, plan)
        steps_b = sum((wide(stage) for stage in range(4)), [])
        contract(steps_b[:LEAD], spread(mixing_in(2), 0, LEAD))
        wait_halo(img, 0, slice(None))
        contract(
            steps_b[LEAD : LEAD + SOAK],
            spread(rows_act(img, halo, range(slabs), affine), 0, SOAK),
        )
        plan = spread(rows_act(img, halo, range(slabs, parts), affine), 0, 2)
        plan.update(spread(kept(0, middle), 3, len(ends_a)))
        contract(ends_a, plan)
        contract(
            steps_b[LEAD + SOAK : LEAD + SOAK + DRAIN],
            spread(
                kept(0, outer) + [functools.partial(prepare_stats, gath_a, lanes_of(0))], 0, DRAIN
            ),
        )
        send_stats(gath_a, 1)
        send_halo(mid, 1, lanes_of(0))
        done = LEAD + SOAK + DRAIN
        plan = spread(mixing_in(3), 0, 5)
        plan.update(spread(
            [functools.partial(split_b, q) for q in range(UNITS)], max(15 - done, 5), 18 - done
        ))
        plan.update(spread(
            [functools.partial(finish_b, 0, 1, 0), functools.partial(finish_b, 1, 2, 0)],
            20 - done, 23 - done,
        ))
        contract(steps_b[done:], plan)
        finish_b(0, 0, 1)
        finish_b(1, height - 1, 1)
        prepare_stats(gath_b, lanes_of(1))
        send_stats(gath_b, 2)
        send_halo(mid, 2, lanes_of(1))

        def give(r, ref):
            for q in range(UNITS):
                lanes = lanes_of(q)
                value = pltpu.matmul_pop(acc[q][ref]) + (part[r, :, lanes] + vec[4:5, lanes])
                out[r, :, lanes] = (img[1 + r, :, lanes].astype(F32) + value).astype(BF16)

        def fold(p, r, first, second, q):
            lanes = lanes_of(q)
            a, b = pltpu.matmul_pop(acc[q][first]), pltpu.matmul_pop(acc[q][second])
            if p == 0:
                part[r, :, lanes] = a + b
                part[r + 1, :, lanes] = a - b
            else:
                part[r, :, lanes] += a + b
                part[r + 1, :, lanes] += a - b

        def save(r, ref):
            for q in range(UNITS):
                part[r, :, lanes_of(q)] += pltpu.matmul_pop(acc[q][ref])

        def product(m, p):
            kind, ref = combos[m][3:]

            def entry(j, q):
                columns = slice(q * SIDE, (q + 1) * SIDE)
                if kind is None:
                    tile = tile_of(w_out, sides[m], j, p, q)
                else:
                    tile = lambda: taps[p, kind, j, :, columns]
                return tile, [(ref, lambda: shifted(mixed, m, j, 0))]

            return [{q: entry(j, q) for q in range(UNITS)} for j in range(3)]

        def second(p, affine):
            here = range(p * slabs, (p + 1) * slabs)
            put = save if p < depth - 1 else give

            def plain(r):
                return [functools.partial(activate_round, mid, r, k, affine) for k in here]

            def mixing(m):
                return [
                    functools.partial(mix_rows, m, *combos[m][:3], k, p * slabs) for k in here
                ]

            def folding(r, first, other):
                return [functools.partial(fold, p, r, first, other, q) for q in range(UNITS)]

            steps = sum((product(m, p) for m in range(8)), [])
            early = spread(mixing(1) + plain(3), 0, 3)
            early.update(spread(mixing(2) + plain(4), 3, 6))
            early.update(spread(mixing(3) + folding(0, 0, 1), 6, 10))
            early.update(spread(mixing(4) + [functools.partial(put, 1, 2)], 10, 13))
            early.update(spread(mixing(5), 13, 15))
            late = spread(plain(0) + mixing(6), 0, 2)
            late.update(spread(plain(5) + folding(2, 3, 0), 2, 4))
            late.update(spread(mixing(7) + [functools.partial(put, 2, 1)], 4, 7))
            late.update({8: [functools.partial(put, 0, 2)]})
            opening = plain(1) + plain(2) + mixing(0)
            if p == depth - 1:
                top, low = plain(0), plain(5)
                early = spread(mixing(1) + plain(3), 0, 3)
                early.update(spread(mixing(2) + plain(4), 3, 6))
                early.update({6: mixing(3)})
                early.update(spread(folding(0, 0, 1), 7, 9))
                late = {
                    0: mixing(4), 1: top[:1], 2: [functools.partial(put, 1, 2)], 3: top[1:],
                    4: mixing(5), 5: low[:1], 6: low[1:] + mixing(6),
                    8: folding(2, 3, 0)[:1], 9: folding(2, 3, 0)[1:] + mixing(7),
                    11: [functools.partial(put, 2, 1)], 14: [functools.partial(put, 0, 2)],
                }
                return opening, steps[:9], early, steps[9:], late, functools.partial(put, height - 1, 3)
            return opening, steps[:15], early, steps[15:], late, functools.partial(put, height - 1, 3)

        def ready(p, gath):
            lanes = lanes_of(p)
            pair = receive_stats(gath, 1 + p, vec[2:3, lanes], vec[3:4, lanes])
            return second(p, affine_of(pair, p * slabs))

        opening, steps, plan, rest, rest_plan, closing = ready(0, gath_a)
        for hook in opening:
            hook()
        contract(steps, plan)
        wait_halo(mid, 1, lanes_of(0))
        contract(rest[:TURN], {t: hooks for t, hooks in rest_plan.items() if t < TURN})
        opening, steps, plan, last, last_plan, final = ready(1, gath_b)
        ahead = len(rest) - TURN
        joined = {t - TURN: list(hooks) for t, hooks in rest_plan.items() if TURN <= t < 8}
        for t, hooks in spread(opening, 0, ahead).items():
            joined.setdefault(t, []).extend(hooks)
        for t, hooks in plan.items():
            joined.setdefault(t + ahead, []).extend(hooks)
        joined[ahead + 1] = joined.get(ahead + 1, []) + rest_plan[8]
        joined[ahead + 3] = joined.get(ahead + 3, []) + [closing]
        contract(rest[TURN:] + steps, joined)
        wait_halo(mid, 2, lanes_of(1))
        contract(last, last_plan)
        final()
        all_sent(gath_in, 0)
        all_sent(gath_a, 1)
        all_sent(gath_b, 2)

    pl.run_scoped(
        body, *[pltpu.ACC(q)((width, SIDE), F32) for q in range(UNITS) for _ in range(height)]
    )


def pin(x):
    return pltpu.with_memory_space_constraint(x, pltpu.HBM)


def local(n, image, gain_in, shift_in, conv_in, gain_mid, shift_mid, conv_out, bias_out):
    height, width, chans = image.shape
    whole = pl.BlockSpec(memory_space=pltpu.HBM)
    operands = (image, gain_in[None], shift_in[None], conv_in, gain_mid[None], shift_mid[None],
                conv_out, bias_out[None])
    return pl.pallas_call(
        functools.partial(kernel, n),
        out_shape=jax.ShapeDtypeStruct(image.shape, image.dtype),
        in_specs=[whole] * len(operands),
        out_specs=pl.BlockSpec(memory_space=pltpu.VMEM),
        scratch_shapes=[
            pltpu.VMEM((height + 2, width, chans), BF16),
            pltpu.VMEM((height + 2, chans // LANES, width + 2 * PAD, LANES), F32),
            pltpu.VMEM((height + 2, width, chans), BF16),
            pltpu.VMEM(conv_in.shape, BF16),
            pltpu.VMEM(conv_out.shape, BF16),
            pltpu.VMEM((2, 3, chans, SIDE), BF16),
            pltpu.VMEM((chans // SIDE, 2, 3, SIDE, chans), BF16),
            pltpu.VMEM((8, chans // LANES, width + 2 * PAD, LANES), F32),
            pltpu.VMEM((height, width, chans), F32),
            pltpu.VMEM((8, chans), F32),
            pltpu.VMEM((2, 8, chans), F32),
            pltpu.VMEM((n, LANES), F32),
            pltpu.VMEM((n, LANES), F32),
            pltpu.VMEM((n, LANES), F32),
            pltpu.SemaphoreType.DMA((height,)),
            pltpu.SemaphoreType.DMA((3,)),
            pltpu.SemaphoreType.DMA((3, 2)),
            pltpu.SemaphoreType.DMA((3, 2)),
            pltpu.SemaphoreType.DMA((3,)),
            pltpu.SemaphoreType.DMA((3,)),
        ],
        compiler_params=pltpu.CompilerParams(
            collective_id=0, has_side_effects=True, vmem_limit_bytes=48 * 1024 * 1024
        ),
    )(*[pin(x) for x in operands])


def solution(mesh):
    n = mesh.shape["rows"]
    in_specs = (P(("img", "rows"), None, None), P(), P(), P(), P(), P(), P(), P())
    out_specs = P(("img", "rows"), None, None)
    return jax.shard_map(
        functools.partial(local, n), mesh=mesh, in_specs=in_specs, out_specs=out_specs,
        check_vma=False,
    )
```

```python
import functools

import jax
import jax.numpy as jnp
from jax import lax
from jax.experimental import pallas as pl
from jax.experimental.pallas import tpu as pltpu
from jax.sharding import PartitionSpec as P

GROUPS = 32
LANES = 128
SIDE = 256
UNITS = 2
CHUNK = 32
PAD = 8
TURN = 5
SOAK = 1
DRAIN = 2
MESH = pl.DeviceIdType.MESH
BF16, F32 = jnp.bfloat16, jnp.float32


def packed(sums, squares):
    chans = sums.shape[1]
    pieces = [part[:, k : k + LANES] for part in (sums, squares) for k in range(0, chans, LANES)]
    return jnp.concatenate(pieces, axis=0)


def flat(tile):
    return jnp.concatenate([tile[k : k + 1] for k in range(tile.shape[0])], axis=1)


def group_total(tile, size):
    lane = lax.broadcasted_iota(jnp.int32, tile.shape, 1)
    step = 1
    while step < size:
        far = min(4, size // step)
        place = (lane // step) % far
        turned = {d: pltpu.roll(tile, (d * step) % LANES, 1) for d in range(1 - far, far) if d}
        total = tile
        for p in range(1, far):
            other = turned[p]
            for d in range(p):
                other = jnp.where(place == d, turned[p - far], other)
            total = total + other
        tile = total
        step *= far
    return tile


def kernel(n, image, gain_in, shift_in, conv_in, gain_mid, shift_mid, conv_out, bias_out, out,
           img, act, mid, w_in, w_out, taps_in, taps, mixed, part, vec, sums, gath_in, gath_a, gath_b,
           img_sem, load_sem, halo_send, halo_recv, stat_send, stat_recv):
    me = lax.axis_index("rows")
    height, width, chans = image.shape
    size = chans // GROUPS
    count = float(height * width * size * n)
    parts = chans // LANES
    depth = chans // SIDE
    slabs = SIDE // LANES
    share = height // UNITS

    order = [0, height - 1] + list(range(1, height - 1))
    loads = {
        r: pltpu.make_async_copy(image.at[r], img.at[1 + r], img_sem.at[r]) for r in order
    }
    for r in order:
        loads[r].start()
    load_w_in = pltpu.make_async_copy(conv_in, w_in, load_sem.at[0])
    load_w_out = pltpu.make_async_copy(conv_out, w_out, load_sem.at[1])

    barrier = pltpu.get_barrier_semaphore()
    for d in range(1, n):
        pl.semaphore_signal(
            barrier, inc=1, device_id={"rows": lax.rem(me + d, n)}, device_id_type=MESH
        )

    def add_stats(value, lanes):
        folded = value.reshape(value.shape[0] // 8, 8, value.shape[1])
        sums[0, :, lanes] += jnp.sum(folded, axis=0)
        sums[1, :, lanes] += jnp.sum(folded * folded, axis=0)

    def stat_copy(gath, which, d):
        return pltpu.make_async_remote_copy(
            src_ref=gath.at[pl.ds(0, 1)],
            dst_ref=gath.at[pl.ds(d, 1)],
            send_sem=stat_send.at[which],
            recv_sem=stat_recv.at[which],
            device_id={"rows": lax.rem(me + d, n)},
            device_id_type=MESH,
        )

    def prepare_stats(gath, lanes):
        tile = packed(
            jnp.sum(sums[0, :, lanes], axis=0, keepdims=True),
            jnp.sum(sums[1, :, lanes], axis=0, keepdims=True),
        )
        tile = group_total(tile, size)
        lane = lax.broadcasted_iota(jnp.int32, tile.shape, 1)
        row = lax.broadcasted_iota(jnp.int32, tile.shape, 0)
        mine = jnp.where(lax.rem(lane, size) == row, tile, 0.0)
        gath[0:1] = jnp.sum(mine, axis=0, keepdims=True)

    def send_stats(gath, which):
        for d in sorted(range(1, n), key=lambda d: min(d, n - d)):
            stat_copy(gath, which, d).start()

    def all_sent(gath, which):
        pltpu.make_async_copy(
            gath.at[pl.ds(1, n - 1)], gath.at[pl.ds(1, n - 1)], stat_send.at[which]
        ).wait()

    def receive_stats(gath, which, gain, shift):
        pltpu.make_async_copy(
            gath.at[pl.ds(1, n - 1)], gath.at[pl.ds(1, n - 1)], stat_recv.at[which]
        ).wait()
        pieces = gain.shape[1] // LANES
        total = jnp.sum(gath[...], axis=0, keepdims=True) * (1.0 / count)
        total = jnp.broadcast_to(total, (2 * pieces, LANES))
        lane = lax.broadcasted_iota(jnp.int32, total.shape, 1)
        row = lax.broadcasted_iota(jnp.int32, total.shape, 0)
        tile = jnp.take_along_axis(total, lane - lax.rem(lane, size) + row, axis=1)
        mean, square = tile[:pieces], tile[pieces:]
        variance = jnp.maximum(square - mean * mean, 0.0)
        scale = flat(lax.rsqrt(variance + 1e-06)) * (0.5 * gain)
        return scale, 0.5 * shift - flat(mean) * scale

    def halo_copies(buf, which, lanes):
        up = pltpu.make_async_remote_copy(
            src_ref=buf.at[1, :, lanes],
            dst_ref=buf.at[height + 1, :, lanes],
            send_sem=halo_send.at[which, 0],
            recv_sem=halo_recv.at[which, 0],
            device_id={"rows": jnp.maximum(me - 1, 0)},
            device_id_type=MESH,
        )
        down = pltpu.make_async_remote_copy(
            src_ref=buf.at[height, :, lanes],
            dst_ref=buf.at[0, :, lanes],
            send_sem=halo_send.at[which, 1],
            recv_sem=halo_recv.at[which, 1],
            device_id={"rows": jnp.minimum(me + 1, n - 1)},
            device_id_type=MESH,
        )
        return up, down

    def send_halo(buf, which, lanes):
        up, down = halo_copies(buf, which, lanes)

        @pl.when(me > 0)
        def _():
            up.start()

        @pl.when(me < n - 1)
        def _():
            down.start()

    def wait_halo(buf, which, lanes):
        up, down = halo_copies(buf, which, lanes)

        @pl.when(me > 0)
        def _():
            up.wait_send()
            down.wait_recv()

        @pl.when(me < n - 1)
        def _():
            down.wait_send()
            up.wait_recv()

    def activated(buf, row, k, affine):
        lanes = slice(k * LANES, (k + 1) * LANES)
        scale, shift = affine[k]
        half = buf[row, :, lanes].astype(F32) * scale + shift
        value = half + half * jnp.tanh(half)
        if row == 0:
            value = jnp.where(me > 0, value, 0.0)
        if row == height + 1:
            value = jnp.where(me < n - 1, value, 0.0)
        return value

    inside = pl.ds(PAD, width)

    def activate(buf, row, k, affine):
        act[row, k, inside] = activated(buf, row, k, affine)

    def activate_round(buf, row, k, affine):
        act[row, k, inside] = activated(buf, row, k, affine).astype(BF16).astype(F32)

    def mix_rows(m, a, b, sign, k, base):
        mixed[m, k - base, inside] = act[a, k, inside] + sign * act[b, k, inside]

    def mix_rounded(m, a, b, sign, k):
        first = act[a, k, inside].astype(BF16).astype(F32)
        mixed[m, k, inside] = first + sign * act[b, k, inside].astype(BF16).astype(F32)

    def shifted(buf, row, j, k):
        cols = pl.ds(PAD + j - 1, width)
        return jnp.concatenate(
            [buf[row, k * slabs + m, cols] for m in range(slabs)], axis=1
        )

    def mix_taps_in(columns):
        def step(t, _):
            rows = pl.ds(pl.multiple_of(t * CHUNK, CHUNK), CHUNK)
            for j in range(3):
                ends = 0.5 * (
                    w_in[0, j, rows, columns].astype(F32) + w_in[2, j, rows, columns].astype(F32)
                )
                centre = 0.5 * w_in[1, j, rows, columns].astype(F32)
                taps_in[0, j, rows] = (ends + centre).astype(BF16)
                taps_in[1, j, rows] = (ends - centre).astype(BF16)
            return 0

        lax.fori_loop(0, chans // CHUNK, step, 0)

    def mix_taps(p):
        def step(t, _):
            rows = pl.ds(pl.multiple_of(t * CHUNK, CHUNK), CHUNK)
            source = pl.ds(pl.multiple_of(p * SIDE + t * CHUNK, CHUNK), CHUNK)
            for j in range(3):
                ends = 0.5 * (
                    w_out[0, j, source].astype(F32) + w_out[2, j, source].astype(F32)
                )
                centre = 0.5 * w_out[1, j, source].astype(F32)
                taps[p, 0, j, rows] = (ends + centre).astype(BF16)
                taps[p, 1, j, rows] = (ends - centre).astype(BF16)
            return 0

        lax.fori_loop(0, SIDE // CHUNK, step, 0)

    def body(*accs):
        acc = [accs[q * height : (q + 1) * height] for q in range(UNITS)]

        zero = jnp.zeros((SIDE, SIDE), BF16)
        for q in range(UNITS):
            for s in range(2):
                pltpu.matmul_acc_lhs(acc[q][0], zero, load_staged_rhs=s)
        for q in range(UNITS):
            for r in range(height):
                pltpu.matmul_pop(acc[q][r])

        def contract(steps, hooks=None):
            def push(t):
                for q, (tile, _) in steps[t].items():
                    pltpu.matmul_push_rhs(tile(), staging_register=t % 2, mxu_index=q)

            push(0)
            for t, step in enumerate(steps):
                if t + 1 < len(steps):
                    push(t + 1)
                for hook in (hooks or {}).get(t, []):
                    hook()
                for m in range(height):
                    for q, (_, pairs) in step.items():
                        if m < len(pairs):
                            ref, left = pairs[m]
                            pltpu.matmul_acc_lhs(
                                acc[q][ref], left(), load_staged_rhs=t % 2 if m == 0 else None
                            )

        def tile_of(weights, i, j, k, p):
            return lambda: weights[
                i, j, k * SIDE : (k + 1) * SIDE, p * SIDE : (p + 1) * SIDE
            ]

        def left_of(j, row, k):
            return lambda: shifted(act, row, j, k)

        spots = [(i, j) for j in range(3) for i in (1, 0, 2)]

        def inner(i, rows):
            return [r for r in rows if 1 <= r + i <= height]

        def place(p, r):
            return r // share, p * share + r % share

        def rows_split(w, p, k):
            def entry(i, j, q):
                rows = inner(i, range(q * share, (q + 1) * share))
                pairs = [(place(p, r)[1], left_of(j, r + i, k)) for r in rows]
                return tile_of(w, i, j, k, p), pairs

            own = [{q: entry(i, j, q) for q in range(UNITS)} for i, j in spots]
            ends = [
                {
                    q: (tile_of(w, i, j, k, p), [(place(p, r)[1], left_of(j, r + i, k))])
                    for q, i, r in ((0, 0, 0), (UNITS - 1, 2, height - 1))
                }
                for j in range(3)
            ]
            return own, ends

        def rows_first(w, p, k):
            queues = []
            for q in range(UNITS):
                rows = list(range(q * share, (q + 1) * share))
                inputs = range(1, height + 1) if q == 0 else range(height, 0, -1)
                queues.append([
                    (tile_of(w, x - r, j, k, p), [(place(p, r)[1], left_of(j, x, k))])
                    for x in inputs
                    for j in range(3)
                    for r in (rows if q == 0 else rows[::-1])
                    if 0 <= x - r <= 2
                ])
            return [dict(enumerate(step)) for step in zip(*queues, strict=True)]

        def spread(hooks, first, last):
            assert first < last
            steps = range(first, last)
            plan = {t: [] for t in steps}
            for m, hook in enumerate(hooks):
                plan[first + m * len(steps) // len(hooks)].append(hook)
            return plan

        def lanes_of(p):
            return slice(p * SIDE, (p + 1) * SIDE)

        def rows_act(buf, rows, ks, affine):
            return [
                functools.partial(activate, buf, r, k, affine) for k in ks for r in rows
            ]

        def affine_of(pair, first=0):
            scale, shift = pair
            return {
                first + k: (scale[:, k * LANES : (k + 1) * LANES], shift[:, k * LANES : (k + 1) * LANES])
                for k in range(scale.shape[1] // LANES)
            }

        mine = range(1, height + 1)
        halo = (0, height + 1)

        sums[...] = jnp.zeros_like(sums)
        for buf in (act, mixed):
            edge = jnp.zeros(buf.shape[:2] + (PAD, LANES), F32)
            buf[:, :, 0:PAD] = edge
            buf[:, :, PAD + width : 2 * PAD + width] = edge

        def stats_step(r, k, _):
            cols = pl.ds(pl.multiple_of(k * CHUNK, CHUNK), CHUNK)
            add_stats(img[1 + r, cols].astype(F32), slice(None))
            return 0

        for r in order:
            loads[r].wait()
            if r == order[-1]:
                for k, source in enumerate((gain_in, shift_in, gain_mid, shift_mid, bias_out)):
                    pltpu.make_async_copy(source, vec.at[pl.ds(k, 1)], load_sem.at[2]).start()
                load_w_in.start()
                load_w_out.start()
            lax.fori_loop(0, width // CHUNK, functools.partial(stats_step, r), 0)
        prepare_stats(gath_in, slice(None))
        pl.semaphore_wait(barrier, n - 1)
        send_stats(gath_in, 0)
        send_halo(img, 0, lanes_of(0))
        send_halo(img, 3, lanes_of(1))
        sums[...] = jnp.zeros_like(sums)
        load_w_in.wait()
        mix_taps_in(slice(SIDE, 2 * SIDE))
        load_w_out.wait()
        for p in range(depth):
            mix_taps(p)
        pltpu.make_async_copy(vec.at[pl.ds(0, 5)], vec.at[pl.ds(0, 5)], load_sem.at[2]).wait()
        affine = affine_of(receive_stats(gath_in, 0, vec[0:1], vec[1:2]))

        def keep(p, r):
            lanes = lanes_of(p)
            q, ref = place(p, r)
            value = pltpu.matmul_pop(acc[q][ref]).astype(BF16)
            mid[1 + r, :, lanes] = value
            add_stats(value.astype(F32), lanes)

        middle = range(1, height - 1)
        outer = (0, height - 1)

        def kept(p, rows):
            return [functools.partial(keep, p, r) for r in rows]

        def both(p):
            first = [rows_split(w_in, p, k) for k in range(depth)]
            return [sum((pair[m] for pair in first), []) for m in range(2)]

        combos = [
            (1, 2, 1.0, 0, 0), (2, 1, -1.0, 1, 1), (3, 1, -1.0, None, 2),
            (3, 4, 1.0, 0, 3), (4, 3, -1.0, 1, 0), (2, 4, -1.0, None, 1),
            (0, 2, -1.0, None, 2), (5, 3, -1.0, None, 3),
        ]
        sides = {2: 2, 5: 0, 6: 0, 7: 2}

        _, ends_a = both(0)
        pairs = ((0, 1, 2, 6), (3, 4, 5, 7))

        def wide(stage):
            ref = (stage + share) % height

            def entry(j, k, q):
                m = pairs[q][stage]
                kind = combos[m][3]
                if kind is None:
                    tile = tile_of(w_in, sides[m], j, k, 1)
                else:
                    tile = lambda: taps_in[kind, j, k * SIDE : (k + 1) * SIDE]
                return tile, [(ref, lambda: shifted(mixed, m, j, k))]

            return [
                {q: entry(j, k, q) for q in range(UNITS)} for k in range(depth) for j in range(3)
            ]

        def mixing_in(stage):
            return [
                functools.partial(mix_rounded, pairs[q][stage], *combos[pairs[q][stage]][:3], k)
                for k in range(parts) for q in range(UNITS)
            ]

        def split_b(q):
            lanes = lanes_of(1)
            a, b = pltpu.matmul_pop(acc[q][share]), pltpu.matmul_pop(acc[q][share + 1])
            part[share * q, :, lanes] = a + b
            part[share * q + 1, :, lanes] = a - b

        def finish_b(q, r, ref):
            lanes = lanes_of(1)
            value = (part[r, :, lanes] + pltpu.matmul_pop(acc[q][ref])).astype(BF16)
            mid[1 + r, :, lanes] = value
            add_stats(value.astype(F32), lanes)

        near = (1, height)
        far = [r for r in mine if r not in near]
        for hook in rows_act(img, near, range(slabs), affine):
            hook()
        start = rows_first(w_in, 0, 0)
        plan = spread(rows_act(img, far, range(slabs), affine), 0, 4)
        plan.update(spread(rows_act(img, mine, range(slabs, parts), affine), 4, len(start)))
        contract(start, plan)
        later = sum((rows_split(w_in, 0, k)[0] for k in range(1, depth)), [])
        plan = spread(mixing_in(0), 0, 5)
        plan.update(spread(mixing_in(1), 5, len(later)))
        contract(later, plan)
        steps_b = sum((wide(stage) for stage in range(4)), [])
        wait_halo(img, 0, lanes_of(0))
        contract(
            steps_b[:SOAK],
            spread(rows_act(img, halo, range(slabs), affine), 0, SOAK),
        )
        wait_halo(img, 3, lanes_of(1))
        plan = spread(rows_act(img, halo, range(slabs, parts), affine), 0, 2)
        plan.update(spread(kept(0, middle), 3, len(ends_a)))
        contract(ends_a, plan)
        contract(
            steps_b[SOAK : SOAK + DRAIN],
            spread(
                kept(0, outer) + [functools.partial(prepare_stats, gath_a, lanes_of(0))], 0, DRAIN
            ),
        )
        send_stats(gath_a, 1)
        send_halo(mid, 1, lanes_of(0))
        done = SOAK + DRAIN
        plan = spread(mixing_in(2), 0, 4)
        plan.update(spread(mixing_in(3), 4, 9))
        plan.update(spread(
            [functools.partial(split_b, q) for q in range(UNITS)], max(15 - done, 5), 18 - done
        ))
        plan.update(spread(
            [functools.partial(finish_b, 0, 1, 0), functools.partial(finish_b, 1, 2, 0)],
            20 - done, 23 - done,
        ))
        contract(steps_b[done:], plan)
        finish_b(0, 0, 1)
        finish_b(1, height - 1, 1)
        prepare_stats(gath_b, lanes_of(1))
        send_stats(gath_b, 2)
        send_halo(mid, 2, lanes_of(1))

        def give(r, ref):
            for q in range(UNITS):
                lanes = lanes_of(q)
                value = pltpu.matmul_pop(acc[q][ref]) + (part[r, :, lanes] + vec[4:5, lanes])
                out[r, :, lanes] = (img[1 + r, :, lanes].astype(F32) + value).astype(BF16)

        def fold(p, r, first, second, q):
            lanes = lanes_of(q)
            a, b = pltpu.matmul_pop(acc[q][first]), pltpu.matmul_pop(acc[q][second])
            if p == 0:
                part[r, :, lanes] = a + b
                part[r + 1, :, lanes] = a - b
            else:
                part[r, :, lanes] += a + b
                part[r + 1, :, lanes] += a - b

        def save(r, ref):
            for q in range(UNITS):
                part[r, :, lanes_of(q)] += pltpu.matmul_pop(acc[q][ref])

        def product(m, p):
            kind, ref = combos[m][3:]

            def entry(j, q):
                columns = slice(q * SIDE, (q + 1) * SIDE)
                if kind is None:
                    tile = tile_of(w_out, sides[m], j, p, q)
                else:
                    tile = lambda: taps[p, kind, j, :, columns]
                return tile, [(ref, lambda: shifted(mixed, m, j, 0))]

            return [{q: entry(j, q) for q in range(UNITS)} for j in range(3)]

        def second(p, affine):
            here = range(p * slabs, (p + 1) * slabs)
            put = save if p < depth - 1 else give

            def plain(r):
                return [functools.partial(activate_round, mid, r, k, affine) for k in here]

            def mixing(m):
                return [
                    functools.partial(mix_rows, m, *combos[m][:3], k, p * slabs) for k in here
                ]

            def folding(r, first, other):
                return [functools.partial(fold, p, r, first, other, q) for q in range(UNITS)]

            steps = sum((product(m, p) for m in range(8)), [])
            early = spread(mixing(1) + plain(3), 0, 3)
            early.update(spread(mixing(2) + plain(4), 3, 6))
            early.update(spread(mixing(3) + folding(0, 0, 1), 6, 10))
            early.update(spread(mixing(4) + [functools.partial(put, 1, 2)], 10, 13))
            early.update(spread(mixing(5), 13, 15))
            late = spread(plain(0) + mixing(6), 0, 2)
            late.update(spread(plain(5) + folding(2, 3, 0), 2, 4))
            late.update(spread(mixing(7) + [functools.partial(put, 2, 1)], 4, 7))
            late.update({8: [functools.partial(put, 0, 2)]})
            opening = plain(1) + plain(2) + mixing(0)
            if p == depth - 1:
                top, low = plain(0), plain(5)
                early = spread(mixing(1) + plain(3), 0, 3)
                early.update(spread(mixing(2) + plain(4), 3, 6))
                early.update({6: mixing(3)})
                early.update(spread(folding(0, 0, 1), 7, 9))
                late = {
                    0: mixing(4), 1: top[:1], 2: [functools.partial(put, 1, 2)], 3: top[1:],
                    4: mixing(5), 5: low[:1], 6: low[1:] + mixing(6),
                    8: folding(2, 3, 0)[:1], 9: folding(2, 3, 0)[1:] + mixing(7),
                    11: [functools.partial(put, 2, 1)], 14: [functools.partial(put, 0, 2)],
                }
                return opening, steps[:9], early, steps[9:], late, functools.partial(put, height - 1, 3)
            return opening, steps[:15], early, steps[15:], late, functools.partial(put, height - 1, 3)

        def ready(p, gath):
            lanes = lanes_of(p)
            pair = receive_stats(gath, 1 + p, vec[2:3, lanes], vec[3:4, lanes])
            return second(p, affine_of(pair, p * slabs))

        opening, steps, plan, rest, rest_plan, closing = ready(0, gath_a)
        for hook in opening:
            hook()
        contract(steps, plan)
        wait_halo(mid, 1, lanes_of(0))
        contract(rest[:TURN], {t: hooks for t, hooks in rest_plan.items() if t < TURN})
        opening, steps, plan, last, last_plan, final = ready(1, gath_b)
        ahead = len(rest) - TURN
        joined = {t - TURN: list(hooks) for t, hooks in rest_plan.items() if TURN <= t < 8}
        for t, hooks in spread(opening, 0, ahead).items():
            joined.setdefault(t, []).extend(hooks)
        for t, hooks in plan.items():
            joined.setdefault(t + ahead, []).extend(hooks)
        joined[ahead + 1] = joined.get(ahead + 1, []) + rest_plan[8]
        joined[ahead + 3] = joined.get(ahead + 3, []) + [closing]
        contract(rest[TURN:] + steps, joined)
        wait_halo(mid, 2, lanes_of(1))
        contract(last, last_plan)
        final()
        all_sent(gath_in, 0)
        all_sent(gath_a, 1)
        all_sent(gath_b, 2)

    pl.run_scoped(
        body, *[pltpu.ACC(q)((width, SIDE), F32) for q in range(UNITS) for _ in range(height)]
    )


def pin(x):
    return pltpu.with_memory_space_constraint(x, pltpu.HBM)


def local(n, image, gain_in, shift_in, conv_in, gain_mid, shift_mid, conv_out, bias_out):
    height, width, chans = image.shape
    whole = pl.BlockSpec(memory_space=pltpu.HBM)
    operands = (image, gain_in[None], shift_in[None], conv_in, gain_mid[None], shift_mid[None],
                conv_out, bias_out[None])
    return pl.pallas_call(
        functools.partial(kernel, n),
        out_shape=jax.ShapeDtypeStruct(image.shape, image.dtype),
        in_specs=[whole] * len(operands),
        out_specs=pl.BlockSpec(memory_space=pltpu.VMEM),
        scratch_shapes=[
            pltpu.VMEM((height + 2, width, chans), BF16),
            pltpu.VMEM((height + 2, chans // LANES, width + 2 * PAD, LANES), F32),
            pltpu.VMEM((height + 2, width, chans), BF16),
            pltpu.VMEM(conv_in.shape, BF16),
            pltpu.VMEM(conv_out.shape, BF16),
            pltpu.VMEM((2, 3, chans, SIDE), BF16),
            pltpu.VMEM((chans // SIDE, 2, 3, SIDE, chans), BF16),
            pltpu.VMEM((8, chans // LANES, width + 2 * PAD, LANES), F32),
            pltpu.VMEM((height, width, chans), F32),
            pltpu.VMEM((8, chans), F32),
            pltpu.VMEM((2, 8, chans), F32),
            pltpu.VMEM((n, LANES), F32),
            pltpu.VMEM((n, LANES), F32),
            pltpu.VMEM((n, LANES), F32),
            pltpu.SemaphoreType.DMA((height,)),
            pltpu.SemaphoreType.DMA((3,)),
            pltpu.SemaphoreType.DMA((4, 2)),
            pltpu.SemaphoreType.DMA((4, 2)),
            pltpu.SemaphoreType.DMA((3,)),
            pltpu.SemaphoreType.DMA((3,)),
        ],
        compiler_params=pltpu.CompilerParams(
            collective_id=0, has_side_effects=True, vmem_limit_bytes=48 * 1024 * 1024
        ),
    )(*[pin(x) for x in operands])


def solution(mesh):
    n = mesh.shape["rows"]
    in_specs = (P(("img", "rows"), None, None), P(), P(), P(), P(), P(), P(), P())
    out_specs = P(("img", "rows"), None, None)
    return jax.shard_map(
        functools.partial(local, n), mesh=mesh, in_specs=in_specs, out_specs=out_specs,
        check_vma=False,
    )
```

```python
import functools

import jax
import jax.numpy as jnp
from jax import lax
from jax.experimental import pallas as pl
from jax.experimental.pallas import tpu as pltpu
from jax.sharding import PartitionSpec as P

GROUPS = 32
LANES = 128
SIDE = 256
UNITS = 2
CHUNK = 32
PAD = 8
LEAD = 1
TURN = 5
SOAK = 1
DRAIN = 3
MESH = pl.DeviceIdType.MESH
BF16, F32 = jnp.bfloat16, jnp.float32


def packed(sums, squares):
    chans = sums.shape[1]
    pieces = [part[:, k : k + LANES] for part in (sums, squares) for k in range(0, chans, LANES)]
    return jnp.concatenate(pieces, axis=0)


def flat(tile):
    return jnp.concatenate([tile[k : k + 1] for k in range(tile.shape[0])], axis=1)


def group_total(tile, size):
    lane = lax.broadcasted_iota(jnp.int32, tile.shape, 1)
    step = 1
    while step < size:
        far = min(4, size // step)
        place = (lane // step) % far
        turned = {d: pltpu.roll(tile, (d * step) % LANES, 1) for d in range(1 - far, far) if d}
        total = tile
        for p in range(1, far):
            other = turned[p]
            for d in range(p):
                other = jnp.where(place == d, turned[p - far], other)
            total = total + other
        tile = total
        step *= far
    return tile


def kernel(n, image, gain_in, shift_in, conv_in, gain_mid, shift_mid, conv_out, bias_out, out,
           img, act, mid, w_in, w_out, taps_in, taps, mixed, part, vec, sums, gath_in, gath_a, gath_b,
           halo_send, halo_recv, stat_send, stat_recv):
    me = lax.axis_index("rows")
    height, width, chans = image.shape
    size = chans // GROUPS
    count = float(height * width * size * n)
    parts = chans // LANES
    depth = chans // SIDE
    slabs = SIDE // LANES
    share = height // UNITS

    barrier = pltpu.get_barrier_semaphore()
    for d in range(1, n):
        pl.semaphore_signal(
            barrier, inc=1, device_id={"rows": lax.rem(me + d, n)}, device_id_type=MESH
        )

    def add_stats(value, lanes):
        folded = value.reshape(value.shape[0] // 8, 8, value.shape[1])
        sums[0, :, lanes] += jnp.sum(folded, axis=0)
        sums[1, :, lanes] += jnp.sum(folded * folded, axis=0)

    def stat_copy(gath, which, d):
        return pltpu.make_async_remote_copy(
            src_ref=gath.at[pl.ds(0, 1)],
            dst_ref=gath.at[pl.ds(d, 1)],
            send_sem=stat_send.at[which],
            recv_sem=stat_recv.at[which],
            device_id={"rows": lax.rem(me + d, n)},
            device_id_type=MESH,
        )

    def prepare_stats(gath, lanes):
        tile = packed(
            jnp.sum(sums[0, :, lanes], axis=0, keepdims=True),
            jnp.sum(sums[1, :, lanes], axis=0, keepdims=True),
        )
        tile = group_total(tile, size)
        lane = lax.broadcasted_iota(jnp.int32, tile.shape, 1)
        row = lax.broadcasted_iota(jnp.int32, tile.shape, 0)
        mine = jnp.where(lax.rem(lane, size) == row, tile, 0.0)
        gath[0:1] = jnp.sum(mine, axis=0, keepdims=True)

    def send_stats(gath, which):
        for d in sorted(range(1, n), key=lambda d: min(d, n - d)):
            stat_copy(gath, which, d).start()

    def all_sent(gath, which):
        pltpu.make_async_copy(
            gath.at[pl.ds(1, n - 1)], gath.at[pl.ds(1, n - 1)], stat_send.at[which]
        ).wait()

    def receive_stats(gath, which, gain, shift):
        pltpu.make_async_copy(
            gath.at[pl.ds(1, n - 1)], gath.at[pl.ds(1, n - 1)], stat_recv.at[which]
        ).wait()
        pieces = gain.shape[1] // LANES
        total = jnp.sum(gath[...], axis=0, keepdims=True) * (1.0 / count)
        total = jnp.broadcast_to(total, (2 * pieces, LANES))
        lane = lax.broadcasted_iota(jnp.int32, total.shape, 1)
        row = lax.broadcasted_iota(jnp.int32, total.shape, 0)
        tile = jnp.take_along_axis(total, lane - lax.rem(lane, size) + row, axis=1)
        mean, square = tile[:pieces], tile[pieces:]
        variance = jnp.maximum(square - mean * mean, 0.0)
        scale = flat(lax.rsqrt(variance + 1e-06)) * (0.5 * gain)
        return scale, 0.5 * shift - flat(mean) * scale

    def halo_copies(buf, which, lanes):
        up = pltpu.make_async_remote_copy(
            src_ref=buf.at[1, :, lanes],
            dst_ref=buf.at[height + 1, :, lanes],
            send_sem=halo_send.at[which, 0],
            recv_sem=halo_recv.at[which, 0],
            device_id={"rows": jnp.maximum(me - 1, 0)},
            device_id_type=MESH,
        )
        down = pltpu.make_async_remote_copy(
            src_ref=buf.at[height, :, lanes],
            dst_ref=buf.at[0, :, lanes],
            send_sem=halo_send.at[which, 1],
            recv_sem=halo_recv.at[which, 1],
            device_id={"rows": jnp.minimum(me + 1, n - 1)},
            device_id_type=MESH,
        )
        return up, down

    def send_halo(buf, which, lanes):
        up, down = halo_copies(buf, which, lanes)

        @pl.when(me > 0)
        def _():
            up.start()

        @pl.when(me < n - 1)
        def _():
            down.start()

    def wait_halo(buf, which, lanes):
        up, down = halo_copies(buf, which, lanes)

        @pl.when(me > 0)
        def _():
            up.wait_send()
            down.wait_recv()

        @pl.when(me < n - 1)
        def _():
            down.wait_send()
            up.wait_recv()

    def activated(buf, row, k, affine):
        lanes = slice(k * LANES, (k + 1) * LANES)
        scale, shift = affine[k]
        half = buf[row, :, lanes].astype(F32) * scale + shift
        value = half + half * jnp.tanh(half)
        if row == 0:
            value = jnp.where(me > 0, value, 0.0)
        if row == height + 1:
            value = jnp.where(me < n - 1, value, 0.0)
        return value

    inside = pl.ds(PAD, width)

    def activate(buf, row, k, affine):
        act[row, k, inside] = activated(buf, row, k, affine)

    def activate_round(buf, row, k, affine):
        act[row, k, inside] = activated(buf, row, k, affine).astype(BF16).astype(F32)

    def mix_rows(m, a, b, sign, k, base):
        mixed[m, k - base, inside] = act[a, k, inside] + sign * act[b, k, inside]

    def mix_rounded(m, a, b, sign, k):
        first = act[a, k, inside].astype(BF16).astype(F32)
        mixed[m, k, inside] = first + sign * act[b, k, inside].astype(BF16).astype(F32)

    def shifted(buf, row, j, k):
        cols = pl.ds(PAD + j - 1, width)
        return jnp.concatenate(
            [buf[row, k * slabs + m, cols] for m in range(slabs)], axis=1
        )

    def mix_taps_in(columns):
        def step(t, _):
            rows = pl.ds(pl.multiple_of(t * CHUNK, CHUNK), CHUNK)
            for j in range(3):
                ends = 0.5 * (
                    w_in[0, j, rows, columns].astype(F32) + w_in[2, j, rows, columns].astype(F32)
                )
                centre = 0.5 * w_in[1, j, rows, columns].astype(F32)
                taps_in[0, j, rows] = (ends + centre).astype(BF16)
                taps_in[1, j, rows] = (ends - centre).astype(BF16)
            return 0

        lax.fori_loop(0, chans // CHUNK, step, 0)

    def mix_taps(p):
        def step(t, _):
            rows = pl.ds(pl.multiple_of(t * CHUNK, CHUNK), CHUNK)
            source = pl.ds(pl.multiple_of(p * SIDE + t * CHUNK, CHUNK), CHUNK)
            for j in range(3):
                ends = 0.5 * (
                    w_out[0, j, source].astype(F32) + w_out[2, j, source].astype(F32)
                )
                centre = 0.5 * w_out[1, j, source].astype(F32)
                taps[p, 0, j, rows] = (ends + centre).astype(BF16)
                taps[p, 1, j, rows] = (ends - centre).astype(BF16)
            return 0

        lax.fori_loop(0, SIDE // CHUNK, step, 0)

    def body(img_sem, load_sem, *accs):
        order = [0, height - 1] + list(range(1, height - 1))
        loads = {
            r: pltpu.make_async_copy(image.at[r], img.at[1 + r], img_sem.at[r]) for r in order
        }
        for r in order:
            loads[r].start()
        load_w_in = pltpu.make_async_copy(conv_in, w_in, load_sem.at[0])
        load_w_out = pltpu.make_async_copy(conv_out, w_out, load_sem.at[1])

        acc = [accs[q * height : (q + 1) * height] for q in range(UNITS)]

        zero = jnp.zeros((SIDE, SIDE), BF16)
        for q in range(UNITS):
            for s in range(2):
                pltpu.matmul_acc_lhs(acc[q][0], zero, load_staged_rhs=s)
        for q in range(UNITS):
            for r in range(height):
                pltpu.matmul_pop(acc[q][r])

        def contract(steps, hooks=None):
            def push(t):
                for q, (tile, _) in steps[t].items():
                    pltpu.matmul_push_rhs(tile(), staging_register=t % 2, mxu_index=q)

            push(0)
            for t, step in enumerate(steps):
                if t + 1 < len(steps):
                    push(t + 1)
                for hook in (hooks or {}).get(t, []):
                    hook()
                for m in range(height):
                    for q, (_, pairs) in step.items():
                        if m < len(pairs):
                            ref, left = pairs[m]
                            pltpu.matmul_acc_lhs(
                                acc[q][ref], left(), load_staged_rhs=t % 2 if m == 0 else None
                            )

        def tile_of(weights, i, j, k, p):
            return lambda: weights[
                i, j, k * SIDE : (k + 1) * SIDE, p * SIDE : (p + 1) * SIDE
            ]

        def left_of(j, row, k):
            return lambda: shifted(act, row, j, k)

        spots = [(i, j) for j in range(3) for i in (1, 0, 2)]

        def inner(i, rows):
            return [r for r in rows if 1 <= r + i <= height]

        def place(p, r):
            return r // share, p * share + r % share

        def rows_split(w, p, k):
            def entry(i, j, q):
                rows = inner(i, range(q * share, (q + 1) * share))
                pairs = [(place(p, r)[1], left_of(j, r + i, k)) for r in rows]
                return tile_of(w, i, j, k, p), pairs

            own = [{q: entry(i, j, q) for q in range(UNITS)} for i, j in spots]
            ends = [
                {
                    q: (tile_of(w, i, j, k, p), [(place(p, r)[1], left_of(j, r + i, k))])
                    for q, i, r in ((0, 0, 0), (UNITS - 1, 2, height - 1))
                }
                for j in range(3)
            ]
            return own, ends

        def rows_first(w, p, k):
            queues = []
            for q in range(UNITS):
                rows = list(range(q * share, (q + 1) * share))
                inputs = range(1, height + 1) if q == 0 else range(height, 0, -1)
                queues.append([
                    (tile_of(w, x - r, j, k, p), [(place(p, r)[1], left_of(j, x, k))])
                    for x in inputs
                    for j in range(3)
                    for r in (rows if q == 0 else rows[::-1])
                    if 0 <= x - r <= 2
                ])
            return [dict(enumerate(step)) for step in zip(*queues, strict=True)]

        def spread(hooks, first, last):
            assert first < last
            steps = range(first, last)
            plan = {t: [] for t in steps}
            for m, hook in enumerate(hooks):
                plan[first + m * len(steps) // len(hooks)].append(hook)
            return plan

        def lanes_of(p):
            return slice(p * SIDE, (p + 1) * SIDE)

        def rows_act(buf, rows, ks, affine):
            return [
                functools.partial(activate, buf, r, k, affine) for k in ks for r in rows
            ]

        def affine_of(pair, first=0):
            scale, shift = pair
            return {
                first + k: (scale[:, k * LANES : (k + 1) * LANES], shift[:, k * LANES : (k + 1) * LANES])
                for k in range(scale.shape[1] // LANES)
            }

        mine = range(1, height + 1)
        halo = (0, height + 1)

        sums[...] = jnp.zeros_like(sums)
        for buf in (act, mixed):
            edge = jnp.zeros(buf.shape[:2] + (PAD, LANES), F32)
            buf[:, :, 0:PAD] = edge
            buf[:, :, PAD + width : 2 * PAD + width] = edge

        def stats_step(r, k, _):
            cols = pl.ds(pl.multiple_of(k * CHUNK, CHUNK), CHUNK)
            add_stats(img[1 + r, cols].astype(F32), slice(None))
            return 0

        for r in order:
            loads[r].wait()
            if r == order[-1]:
                for k, source in enumerate((gain_in, shift_in, gain_mid, shift_mid, bias_out)):
                    pltpu.make_async_copy(source, vec.at[pl.ds(k, 1)], load_sem.at[2]).start()
                load_w_in.start()
                load_w_out.start()
            lax.fori_loop(0, width // CHUNK, functools.partial(stats_step, r), 0)
        prepare_stats(gath_in, slice(None))
        pl.semaphore_wait(barrier, n - 1)
        send_stats(gath_in, 0)
        send_halo(img, 0, slice(None))
        sums[...] = jnp.zeros_like(sums)
        load_w_in.wait()
        mix_taps_in(slice(SIDE, 2 * SIDE))
        load_w_out.wait()
        for p in range(depth):
            mix_taps(p)
        pltpu.make_async_copy(vec.at[pl.ds(0, 5)], vec.at[pl.ds(0, 5)], load_sem.at[2]).wait()
        affine = affine_of(receive_stats(gath_in, 0, vec[0:1], vec[1:2]))

        def keep(p, r):
            lanes = lanes_of(p)
            q, ref = place(p, r)
            value = pltpu.matmul_pop(acc[q][ref]).astype(BF16)
            mid[1 + r, :, lanes] = value
            add_stats(value.astype(F32), lanes)

        middle = range(1, height - 1)
        outer = (0, height - 1)

        def kept(p, rows):
            return [functools.partial(keep, p, r) for r in rows]

        def both(p):
            first = [rows_split(w_in, p, k) for k in range(depth)]
            return [sum((pair[m] for pair in first), []) for m in range(2)]

        combos = [
            (1, 2, 1.0, 0, 0), (2, 1, -1.0, 1, 1), (3, 1, -1.0, None, 2),
            (3, 4, 1.0, 0, 3), (4, 3, -1.0, 1, 0), (2, 4, -1.0, None, 1),
            (0, 2, -1.0, None, 2), (5, 3, -1.0, None, 3),
        ]
        sides = {2: 2, 5: 0, 6: 0, 7: 2}

        _, ends_a = both(0)
        pairs = ((0, 1, 2, 6), (3, 4, 5, 7))

        def wide(stage):
            ref = (stage + share) % height

            def entry(j, k, q):
                m = pairs[q][stage]
                kind = combos[m][3]
                if kind is None:
                    tile = tile_of(w_in, sides[m], j, k, 1)
                else:
                    tile = lambda: taps_in[kind, j, k * SIDE : (k + 1) * SIDE]
                return tile, [(ref, lambda: shifted(mixed, m, j, k))]

            return [
                {q: entry(j, k, q) for q in range(UNITS)} for k in range(depth) for j in range(3)
            ]

        def mixing_in(stage):
            return [
                functools.partial(mix_rounded, pairs[q][stage], *combos[pairs[q][stage]][:3], k)
                for k in range(parts) for q in range(UNITS)
            ]

        def split_b(q):
            lanes = lanes_of(1)
            a, b = pltpu.matmul_pop(acc[q][share]), pltpu.matmul_pop(acc[q][share + 1])
            part[share * q, :, lanes] = a + b
            part[share * q + 1, :, lanes] = a - b

        def finish_b(q, r, ref):
            lanes = lanes_of(1)
            value = (part[r, :, lanes] + pltpu.matmul_pop(acc[q][ref])).astype(BF16)
            mid[1 + r, :, lanes] = value
            add_stats(value.astype(F32), lanes)

        near = (1, height)
        far = [r for r in mine if r not in near]
        for hook in rows_act(img, near, range(slabs), affine):
            hook()
        start = rows_first(w_in, 0, 0)
        plan = spread(rows_act(img, far, range(slabs), affine), 0, 4)
        plan.update(spread(rows_act(img, mine, range(slabs, parts), affine), 4, len(start)))
        contract(start, plan)
        later = sum((rows_split(w_in, 0, k)[0] for k in range(1, depth)), [])
        plan = spread(mixing_in(0), 0, 5)
        plan.update(spread(mixing_in(1), 5, len(later)))
        contract(later, plan)
        steps_b = sum((wide(stage) for stage in range(4)), [])
        contract(steps_b[:LEAD], spread(mixing_in(2), 0, LEAD))
        wait_halo(img, 0, slice(None))
        contract(
            steps_b[LEAD : LEAD + SOAK],
            spread(rows_act(img, halo, range(slabs), affine), 0, SOAK),
        )
        plan = spread(rows_act(img, halo, range(slabs, parts), affine), 0, 2)
        plan.update(spread(kept(0, middle), 3, len(ends_a)))
        contract(ends_a, plan)
        contract(
            steps_b[LEAD + SOAK : LEAD + SOAK + DRAIN],
            spread(
                kept(0, outer) + [functools.partial(prepare_stats, gath_a, lanes_of(0))], 0, DRAIN
            ),
        )
        send_stats(gath_a, 1)
        send_halo(mid, 1, lanes_of(0))
        done = LEAD + SOAK + DRAIN
        plan = spread(mixing_in(3), 0, 5)
        plan.update(spread(
            [functools.partial(split_b, q) for q in range(UNITS)], max(15 - done, 5), 18 - done
        ))
        plan.update(spread(
            [functools.partial(finish_b, 0, 1, 0), functools.partial(finish_b, 1, 2, 0)],
            20 - done, 23 - done,
        ))
        contract(steps_b[done:], plan)
        finish_b(0, 0, 1)
        finish_b(1, height - 1, 1)
        prepare_stats(gath_b, lanes_of(1))
        send_stats(gath_b, 2)
        send_halo(mid, 2, lanes_of(1))

        def give(r, ref):
            for q in range(UNITS):
                lanes = lanes_of(q)
                value = pltpu.matmul_pop(acc[q][ref]) + (part[r, :, lanes] + vec[4:5, lanes])
                out[r, :, lanes] = (img[1 + r, :, lanes].astype(F32) + value).astype(BF16)

        def fold(p, r, first, second, q):
            lanes = lanes_of(q)
            a, b = pltpu.matmul_pop(acc[q][first]), pltpu.matmul_pop(acc[q][second])
            if p == 0:
                part[r, :, lanes] = a + b
                part[r + 1, :, lanes] = a - b
            else:
                part[r, :, lanes] += a + b
                part[r + 1, :, lanes] += a - b

        def save(r, ref):
            for q in range(UNITS):
                part[r, :, lanes_of(q)] += pltpu.matmul_pop(acc[q][ref])

        def product(m, p):
            kind, ref = combos[m][3:]

            def entry(j, q):
                columns = slice(q * SIDE, (q + 1) * SIDE)
                if kind is None:
                    tile = tile_of(w_out, sides[m], j, p, q)
                else:
                    tile = lambda: taps[p, kind, j, :, columns]
                return tile, [(ref, lambda: shifted(mixed, m, j, 0))]

            return [{q: entry(j, q) for q in range(UNITS)} for j in range(3)]

        def second(p, affine):
            here = range(p * slabs, (p + 1) * slabs)
            put = save if p < depth - 1 else give

            def plain(r):
                return [functools.partial(activate_round, mid, r, k, affine) for k in here]

            def mixing(m):
                return [
                    functools.partial(mix_rows, m, *combos[m][:3], k, p * slabs) for k in here
                ]

            def folding(r, first, other):
                return [functools.partial(fold, p, r, first, other, q) for q in range(UNITS)]

            steps = sum((product(m, p) for m in range(8)), [])
            early = spread(mixing(1) + plain(3), 0, 3)
            early.update(spread(mixing(2) + plain(4), 3, 6))
            early.update(spread(mixing(3) + folding(0, 0, 1), 6, 10))
            early.update(spread(mixing(4) + [functools.partial(put, 1, 2)], 10, 13))
            early.update(spread(mixing(5), 13, 15))
            late = spread(plain(0) + mixing(6), 0, 2)
            late.update(spread(plain(5) + folding(2, 3, 0), 2, 4))
            late.update(spread(mixing(7) + [functools.partial(put, 2, 1)], 4, 7))
            late.update({8: [functools.partial(put, 0, 2)]})
            opening = plain(1) + plain(2) + mixing(0)
            if p == depth - 1:
                top, low = plain(0), plain(5)
                early = spread(mixing(1) + plain(3), 0, 3)
                early.update(spread(mixing(2) + plain(4), 3, 6))
                early.update({6: mixing(3)})
                early.update(spread(folding(0, 0, 1), 7, 9))
                late = {
                    0: mixing(4), 1: top[:1], 2: [functools.partial(put, 1, 2)], 3: top[1:],
                    4: mixing(5), 5: low[:1], 6: low[1:] + mixing(6),
                    8: folding(2, 3, 0)[:1], 9: folding(2, 3, 0)[1:] + mixing(7),
                    11: [functools.partial(put, 2, 1)], 14: [functools.partial(put, 0, 2)],
                }
                return opening, steps[:9], early, steps[9:], late, functools.partial(put, height - 1, 3)
            return opening, steps[:15], early, steps[15:], late, functools.partial(put, height - 1, 3)

        def ready(p, gath):
            lanes = lanes_of(p)
            pair = receive_stats(gath, 1 + p, vec[2:3, lanes], vec[3:4, lanes])
            return second(p, affine_of(pair, p * slabs))

        opening, steps, plan, rest, rest_plan, closing = ready(0, gath_a)
        for hook in opening:
            hook()
        contract(steps, plan)
        wait_halo(mid, 1, lanes_of(0))
        contract(rest[:TURN], {t: hooks for t, hooks in rest_plan.items() if t < TURN})
        opening, steps, plan, last, last_plan, final = ready(1, gath_b)
        ahead = len(rest) - TURN
        joined = {t - TURN: list(hooks) for t, hooks in rest_plan.items() if TURN <= t < 8}
        for t, hooks in spread(opening, 0, ahead).items():
            joined.setdefault(t, []).extend(hooks)
        for t, hooks in plan.items():
            joined.setdefault(t + ahead, []).extend(hooks)
        joined[ahead + 1] = joined.get(ahead + 1, []) + rest_plan[8]
        joined[ahead + 3] = joined.get(ahead + 3, []) + [closing]
        contract(rest[TURN:] + steps, joined)
        wait_halo(mid, 2, lanes_of(1))
        contract(last, last_plan)
        final()
        all_sent(gath_in, 0)
        all_sent(gath_a, 1)
        all_sent(gath_b, 2)

    pl.run_scoped(
        body,
        pltpu.SemaphoreType.DMA((height,)),
        pltpu.SemaphoreType.DMA((3,)),
        *[pltpu.ACC(q)((width, SIDE), F32) for q in range(UNITS) for _ in range(height)],
    )


def pin(x):
    return pltpu.with_memory_space_constraint(x, pltpu.HBM)


def local(n, image, gain_in, shift_in, conv_in, gain_mid, shift_mid, conv_out, bias_out):
    height, width, chans = image.shape
    whole = pl.BlockSpec(memory_space=pltpu.HBM)
    operands = (image, gain_in[None], shift_in[None], conv_in, gain_mid[None], shift_mid[None],
                conv_out, bias_out[None])
    return pl.pallas_call(
        functools.partial(kernel, n),
        out_shape=jax.ShapeDtypeStruct(image.shape, image.dtype),
        in_specs=[whole] * len(operands),
        out_specs=pl.BlockSpec(memory_space=pltpu.VMEM),
        scratch_shapes=[
            pltpu.VMEM((height + 2, width, chans), BF16),
            pltpu.VMEM((height + 2, chans // LANES, width + 2 * PAD, LANES), F32),
            pltpu.VMEM((height + 2, width, chans), BF16),
            pltpu.VMEM(conv_in.shape, BF16),
            pltpu.VMEM(conv_out.shape, BF16),
            pltpu.VMEM((2, 3, chans, SIDE), BF16),
            pltpu.VMEM((chans // SIDE, 2, 3, SIDE, chans), BF16),
            pltpu.VMEM((8, chans // LANES, width + 2 * PAD, LANES), F32),
            pltpu.VMEM((height, width, chans), F32),
            pltpu.VMEM((8, chans), F32),
            pltpu.VMEM((2, 8, chans), F32),
            pltpu.VMEM((n, LANES), F32),
            pltpu.VMEM((n, LANES), F32),
            pltpu.VMEM((n, LANES), F32),
            pltpu.SemaphoreType.DMA((3, 2)),
            pltpu.SemaphoreType.DMA((3, 2)),
            pltpu.SemaphoreType.DMA((3,)),
            pltpu.SemaphoreType.DMA((3,)),
        ],
        compiler_params=pltpu.CompilerParams(
            collective_id=0, has_side_effects=True, vmem_limit_bytes=48 * 1024 * 1024
        ),
    )(*[pin(x) for x in operands])


def solution(mesh):
    n = mesh.shape["rows"]
    in_specs = (P(("img", "rows"), None, None), P(), P(), P(), P(), P(), P(), P())
    out_specs = P(("img", "rows"), None, None)
    return jax.shard_map(
        functools.partial(local, n), mesh=mesh, in_specs=in_specs, out_specs=out_specs,
        check_vma=False,
    )
```
